32 devices in a mesh: groups: 2 (over y), row: 4 (over z), col: 4 (over x, core).
Axes of the slice: x: 2, y: 2, z: 4, core: 2. Of those that a mesh axis runs over, the one named last changes fastest.
Arguments:
- positions: float32 [2, 8, 4, 512], P(None, ('groups', 'row'), 'col'), parts along dimension 1, may hold values from 0 to 1
- genes: int32 [8, 4, 512], P(('groups', 'row'), 'col'), parts along dimension 0, may hold values from 0 to 479
- candidates: int32 [8, 4, 512, 128], P(('groups', 'row'), 'col'), parts along dimension 0, may hold values from 0 to 1151, as said below
- block_counts: int32 [8, 4, 2], P(('groups', 'row'), 'col'), parts along dimension 0, may hold values from 0 to 256, as said below
- profile_weights: float32 [480, 8, 4, 128], P(None, ('groups', 'row'), 'col'), parts along dimension 1, may hold values from 0.05 to 5
- centroids: float32 [2, 8, 4, 128], P(None, ('groups', 'row'), 'col'), parts along dimension 1, may hold values from 0 to 1
- spreads: float32 [2, 8, 4, 128], P(None, ('groups', 'row'), 'col'), parts along dimension 1, may hold values from 0.05 to 0.4
- correlation: float32 [8, 4, 128], P(('groups', 'row'), 'col'), parts along dimension 0, may hold values from -0.6 to 0.6
Outputs:
- final_profile: float32 [480, 8, 4, 128], P(None, ('groups', 'row'), 'col'), parts along dimension 1
- final_cells: float32 [6, 8, 4, 128], P(None, ('groups', 'row'), 'col'), parts along dimension 1
The draws below stay inside these ranges and needn't reach their ends.
There are 2 independent parts, one for each index of `groups`. The reference program is written for one: setup_inputs(seed, part) draws one part's arguments, and reference() takes and returns one part's arrays. A program takes and returns all parts, laid end to end along the dimension named above; each array names one. Nothing has to cross between parts.
Inputs may be any that keep to these rules, and one draw needn't show every extreme that they name: `candidates`: every candidate names a cell of the transcript's own tile or of one of the eight tiles around it that lie in the slab; an id may appear more than once in one list. `block_counts`: in each tile the blocks with a nonzero count come first, and the first block of every tile is full.
All inputs are finite; a program needn't handle non-finite values.
Results may differ from the reference program's by a relative error of at most 0.0003.
Values sent between devices are 32-bit elements; how exact they have to be, the bound alone decides.
No kernel may reach another device: no remote copies, remote signals or barrier semaphores. Data moves between devices by JAX's collectives and lax.ppermute only.
A program may use at most 64 MiB of HBM per device.

```python
import math
import jax
import jax.numpy as jnp
import numpy as np
from jax import lax

G = 480
K = 128
CAND = 128
BLOCK = 256
NBLK = 2
ITERS = 2
TILE_ROWS = 4
TILE_COLS = 4
TOK = 512


def draw_candidates(key, part):
    key_row, key_col, key_cell = jax.random.split(key, 3)
    grid_shape = (TILE_ROWS, TILE_COLS, TOK, CAND)
    step_row = jax.random.randint(key_row, grid_shape, -1, 2)
    step_col = jax.random.randint(key_col, grid_shape, -1, 2)
    within = jax.random.randint(key_cell, grid_shape, 0, K)
    row_here = jnp.arange(TILE_ROWS, dtype=jnp.int32)[:, None, None, None]
    col_here = jnp.arange(TILE_COLS, dtype=jnp.int32)[None, :, None, None]
    home_row = jnp.clip(row_here + step_row, 0, TILE_ROWS - 1)
    home_col = jnp.clip(col_here + step_col, 0, TILE_COLS - 1)
    neighbour_slot = (home_row - row_here + 1) * 3 + (home_col - col_here + 1)
    return (neighbour_slot * K + within).astype(jnp.int32)


def draw_block_counts(key, part):
    key_live, key_filled = jax.random.split(key, 2)
    live_count = jax.random.randint(key_live, (TILE_ROWS, TILE_COLS, 1), 1, NBLK + 1)
    live_count = live_count.at[0, 0, 0].set(NBLK)
    filled = jax.random.randint(key_filled, (TILE_ROWS, TILE_COLS, NBLK), BLOCK // 4, BLOCK + 1)
    filled = filled.at[:, :, 0].set(BLOCK)
    block_ids = jnp.arange(NBLK, dtype=jnp.int32)[None, None, :]
    return jnp.where(block_ids < live_count, filled, 0).astype(jnp.int32)


def touch_ends(array, stream_key, smallest, largest):
    longest = array.shape.index(max(array.shape))
    spots = []
    for shift in (0, 1):
        where = [jax.random.randint(jax.random.fold_in(stream_key, axis), (), 0, length) for axis, length in enumerate(array.shape)]
        where[longest] = (where[longest] + shift) % array.shape[longest]
        spots.append(tuple(where))
    return array.at[spots[0]].set(smallest).at[spots[1]].set(largest)


def level_of(key, shape, shards, smallest, largest):
    level, own = 1.0, jax.random.fold_in(key, 6)
    for axis_at, blocks in shards:
        steps = jnp.exp(jax.random.uniform(jax.random.fold_in(own, axis_at), (blocks,), jnp.float32, smallest / len(shards), largest / len(shards)))
        level = level * jnp.repeat(steps, shape[axis_at] // blocks).reshape([-1 if axis == axis_at else 1 for axis in range(len(shape))])
    return level


def rank_table(amount, slope):
    loads = [(1 << 20) // math.isqrt(grade ** slope) + 1 for grade in range(1, amount + 1)]
    spread = 1 + sum(loads) // (1 << 30)
    return np.cumsum(np.array([max(1, weight // spread) for weight in loads]))


def ranked_ids(own_key, extent, amount, lean):
    table = rank_table(amount, lean)
    pick = jax.random.randint(jax.random.fold_in(own_key, 1), extent, 0, int(table[amount - 1]))
    grade = jnp.searchsorted(jnp.asarray(table, jnp.int32), pick, side="right")
    return jax.random.permutation(jax.random.fold_in(own_key, 2), amount)[grade].astype(jnp.int32)


def setup_inputs(seed: int = 0, part: int = 0) -> dict:
    key_of = jax.random.split(jax.random.key(seed), 9)
    own_keys = jax.random.split(jax.random.fold_in(key_of[8], part), 9)
    return {
        "positions": jnp.clip(1.0 * jax.random.uniform(own_keys[0], (2, TILE_ROWS, TILE_COLS, TOK), jnp.float32) ** level_of(own_keys[0], (2, TILE_ROWS, TILE_COLS, TOK), ((1, 4), (2, 4)), -0.2, 0.2), 0.0, 1.0),
        "genes": touch_ends(ranked_ids(own_keys[1], (TILE_ROWS, TILE_COLS, TOK), G, 2), jax.random.fold_in(own_keys[1], 3), 0, G - 1).astype(jnp.int32),
        "candidates": draw_candidates(jax.random.fold_in(jax.random.fold_in(key_of[8], part), 71), part),
        "block_counts": draw_block_counts(jax.random.fold_in(jax.random.fold_in(key_of[8], part), 71), part),
        "profile_weights": jnp.clip(jnp.exp(math.log(5.0) - 4.6051702 * jax.random.uniform(own_keys[4], (G, TILE_ROWS, TILE_COLS, K), jnp.float32) ** level_of(own_keys[4], (G, TILE_ROWS, TILE_COLS, K), ((1, 4), (2, 4)), -0.2, 0.2)), 0.05, 5.0),
        "centroids": jnp.clip(1.0 * jax.random.uniform(own_keys[5], (2, TILE_ROWS, TILE_COLS, K), jnp.float32) ** level_of(own_keys[5], (2, TILE_ROWS, TILE_COLS, K), ((1, 4), (2, 4)), -0.2, 0.2), 0.0, 1.0),
        "spreads": jnp.clip(jnp.exp(math.log(0.4) - 2.0794415 * jax.random.uniform(own_keys[6], (2, TILE_ROWS, TILE_COLS, K), jnp.float32) ** level_of(own_keys[6], (2, TILE_ROWS, TILE_COLS, K), ((1, 4), (2, 4)), -0.2, 0.2)), 0.05, 0.4),
        "correlation": jnp.clip(jax.random.uniform(own_keys[7], (TILE_ROWS, TILE_COLS, K), jnp.float32, -0.6, 0.6) * level_of(own_keys[7], (TILE_ROWS, TILE_COLS, K), ((0, 4), (1, 4)), -0.4, 0.0), -0.6, 0.6),
    }


pseudo_count = 0.05
prior_weight = 1.0

def cell_terms(profile, cov_rr, cov_rc, cov_cc, log_weight):
    determinant = cov_rr * cov_cc - cov_rc * cov_rc
    return (jnp.log(profile), cov_cc / determinant, -cov_rc / determinant, cov_rr / determinant, log_weight - 0.5 * jnp.log(determinant))

def update_cells(gene_counts, moments, centre_row, centre_col, cov_rr, cov_rc, cov_cc):
    weight_sum, sum_row, sum_col, sum_rr, sum_rc, sum_cc = moments
    gene_total = gene_counts.shape[0]
    profile = (gene_counts + pseudo_count) / (lax.optimization_barrier(jnp.sum(gene_counts, axis=0)) + gene_total * pseudo_count)
    new_row = (sum_row + prior_weight * centre_row) / (weight_sum + prior_weight)
    new_col = (sum_col + prior_weight * centre_col) / (weight_sum + prior_weight)
    scatter_rr = sum_rr - 2.0 * new_row * sum_row + weight_sum * new_row * new_row
    scatter_rc = sum_rc - new_row * sum_col - new_col * sum_row + weight_sum * new_row * new_col
    scatter_cc = sum_cc - 2.0 * new_col * sum_col + weight_sum * new_col * new_col
    denominator = weight_sum + prior_weight
    return (profile, new_row, new_col, (scatter_rr + prior_weight * cov_rr) / denominator, (scatter_rc + prior_weight * cov_rc) / denominator, (scatter_cc + prior_weight * cov_cc) / denominator, jnp.log(weight_sum + 1.0))

def cell_summary(centre_row, centre_col, cov_rr, cov_rc, cov_cc, log_weight):
    return jnp.stack([centre_row, centre_col, 0.5 * jnp.log(cov_rr), 0.5 * jnp.log(cov_cc), cov_rc / jnp.sqrt(cov_rr * cov_cc), log_weight])

def reference(positions, genes, candidates, block_counts, profile_weights, centroids, spreads, correlation):
    gene_total, tile_rows, tile_cols, tile_cells = profile_weights.shape
    cell_count = tile_rows * tile_cols * tile_cells
    tile_tokens = genes.shape[2]
    profile = (profile_weights / lax.optimization_barrier(jnp.sum(profile_weights, axis=0, keepdims=True))).reshape(gene_total, cell_count)
    centre_row = centroids[0].reshape(cell_count)
    centre_col = centroids[1].reshape(cell_count)
    spread_row = spreads[0].reshape(cell_count)
    spread_col = spreads[1].reshape(cell_count)
    cov_rr = spread_row * spread_row
    cov_cc = spread_col * spread_col
    cov_rc = correlation.reshape(cell_count) * spread_row * spread_col
    log_weight = jnp.zeros((cell_count,), jnp.float32)
    tile_of_cell = jnp.arange(cell_count, dtype=jnp.int32) // tile_cells
    home_row = tile_of_cell // tile_cols
    home_col = tile_of_cell % tile_cols
    token_ids = jnp.arange(tile_tokens, dtype=jnp.int32)
    valid_rows = ((token_ids % BLOCK)[None, None, :] < block_counts[:, :, token_ids // BLOCK]).astype(jnp.float32)
    column_ids = jnp.arange(tile_cols, dtype=jnp.int32)[:, None, None]
    slot_ids = jnp.arange(CAND, dtype=jnp.int32)
    earlier = slot_ids[None, :] < slot_ids[:, None]
    for iteration in range(ITERS):
        log_table, prec_rr, prec_rc, prec_cc, cell_bias = cell_terms(profile, cov_rr, cov_rc, cov_cc, log_weight)

        def tile_row(accum, row_index):
            count_acc, moment_acc = accum
            local_ids = candidates[row_index]
            neighbour_slot = local_ids // tile_cells
            cand_row = row_index + neighbour_slot // 3 - 1
            cand_col = column_ids + neighbour_slot % 3 - 1
            candidate_ids = ((cand_row * tile_cols + cand_col) * tile_cells + local_ids % tile_cells).astype(jnp.int32)
            pos_row = positions[0, row_index][..., None]
            pos_col = positions[1, row_index][..., None]
            gene_row = genes[row_index][..., None]
            shift_row = (home_row[candidate_ids] - row_index).astype(jnp.float32)
            shift_col = (home_col[candidate_ids] - column_ids).astype(jnp.float32)
            delta_row = pos_row - (centre_row[candidate_ids] + shift_row)
            delta_col = pos_col - (centre_col[candidate_ids] + shift_col)
            score = log_table[gene_row, candidate_ids] + cell_bias[candidate_ids] - 0.5 * (prec_rr[candidate_ids] * delta_row * delta_row + 2.0 * prec_rc[candidate_ids] * delta_row * delta_col + prec_cc[candidate_ids] * delta_col * delta_col)
            row_max = lax.optimization_barrier(jnp.max(score, axis=-1, keepdims=True))
            exp_terms = jnp.exp(score - row_max)
            posterior = exp_terms / lax.optimization_barrier(jnp.sum(exp_terms, axis=-1, keepdims=True)) * valid_rows[row_index][..., None]
            same_cell = candidate_ids[..., :, None] == candidate_ids[..., None, :]
            joint_share = lax.optimization_barrier(jnp.sum(jnp.where(same_cell, posterior[..., None, :], 0.0), axis=-1))
            repeat = jnp.any(same_cell & earlier, axis=-1)
            rounded_share = lax.optimization_barrier(joint_share.astype(jnp.bfloat16)).astype(jnp.float32)
            rounded_share = jnp.where(repeat, 0.0, rounded_share)
            count_acc = count_acc.at[gene_row, candidate_ids].add(rounded_share)
            local_row = pos_row - shift_row
            local_col = pos_col - shift_col
            moment_terms = jnp.stack([posterior, posterior * local_row, posterior * local_col, posterior * local_row * local_row, posterior * local_row * local_col, posterior * local_col * local_col])
            moment_acc = moment_acc.at[:, candidate_ids].add(moment_terms)
            return ((count_acc, moment_acc), None)
        start_acc = (jnp.zeros((gene_total, cell_count), jnp.float32), jnp.zeros((6, cell_count), jnp.float32))
        (gene_counts, moments), _ = lax.scan(tile_row, start_acc, jnp.arange(tile_rows, dtype=jnp.int32))
        profile, centre_row, centre_col, cov_rr, cov_rc, cov_cc, log_weight = update_cells(gene_counts, tuple((moments[member] for member in range(6))), centre_row, centre_col, cov_rr, cov_rc, cov_cc)
    final_profile = jnp.log(profile).reshape(gene_total, tile_rows, tile_cols, tile_cells)
    final_cells = cell_summary(centre_row, centre_col, cov_rr, cov_rc, cov_cc, log_weight)
    return (final_profile, final_cells.reshape(6, tile_rows, tile_cols, tile_cells))
```

```python
import functools

import jax
import jax.numpy as jnp
from jax import lax
from jax.experimental import pallas as pl
from jax.experimental.pallas import tpu as pltpu
from jax.sharding import PartitionSpec as P

BLOCK = 256
ITERS = 2
LANES = 128
FEATURES = 8
PARTS = 3
NEVER = -1e30

pseudo_count = 0.05
prior_weight = 1.0

f32 = jnp.float32
bf16 = jnp.bfloat16
i32 = jnp.int32


def shifted(x, axis, by):
    count = lax.axis_size(axis)
    pairs = [(i, i + by) for i in range(count) if 0 <= i + by < count]
    return lax.ppermute(x, axis, pairs)


def params(mib=40):
    return pltpu.CompilerParams(vmem_limit_bytes=mib << 20)


def cost(flops, size):
    return pl.CostEstimate(flops=flops, bytes_accessed=size, transcendentals=0)


def call(kernel, name, outs, in_specs, scratch, flops, args):
    shapes = [jax.ShapeDtypeStruct(s, d) for s, d in outs]
    return pl.pallas_call(
        kernel,
        name=name,
        out_shape=shapes,
        in_specs=in_specs,
        out_specs=[pl.BlockSpec(memory_space=pltpu.VMEM)] * len(shapes),
        scratch_shapes=scratch,
        compiler_params=params(),
        cost_estimate=cost(flops, 1 << 20),
    )(*args)


VMEM = pl.BlockSpec(memory_space=pltpu.VMEM)
SMEM = pl.BlockSpec(memory_space=pltpu.SMEM)


def lane_tile(k):
    return pl.ds(k * LANES, LANES)


def pack_kernel(count_ref, cand_ref, pos_ref, gene_ref, out_ref):
    tokens, slots = cand_ref.shape
    tiles = tokens // LANES
    out_ref[0:slots, :] = cand_ref[...].astype(f32).T
    lane = lax.broadcasted_iota(i32, (1, LANES), 1)
    for k in range(tiles):
        start = k * LANES
        live = (start % BLOCK + lane) < count_ref[start // BLOCK]
        rows = [
            pos_ref[k : k + 1, :],
            pos_ref[tiles + k : tiles + k + 1, :],
            gene_ref[k : k + 1, :].astype(f32),
            live.astype(f32),
            jnp.zeros((FEATURES - 4, LANES), f32),
        ]
        out_ref[slots : slots + FEATURES, lane_tile(k)] = jnp.concatenate(rows, axis=0)


def multiple_kernel(tile_cells, up_ref, own_ref, down_ref, left_ref, mid_ref, right_ref, word_s, unit_s):
    rows, tokens = own_ref.shape
    slots = rows - FEATURES
    words = tile_cells // 8
    shift = tile_cells.bit_length() - 1
    word_shift = words.bit_length() - 1
    held = 3 * words // 8
    per_tile = words // 8
    sub = lax.broadcasted_iota(i32, (8, LANES), 0)
    outs = (left_ref, mid_ref, right_ref)
    nibbles = jnp.full((8, LANES), 0x0F0F0F0F, i32)
    for source, z_ref in enumerate((up_ref, own_ref, down_ref)):
        for k in range(tokens // LANES):
            local = z_ref[0:slots, lane_tile(k)].astype(i32) - (2 - source) * 3 * tile_cells
            word_s[k] = (local >> shift) * words + (local & (words - 1))
            unit_s[k] = 1 << (((local & (tile_cells - 1)) >> word_shift) * 4)
        for k in range(tokens // LANES):

            def group(g, carry):
                low, high = carry
                word = [jnp.zeros((8, LANES), i32) for _ in range(held)]
                for j in range(8):
                    which = word_s[k, pl.ds(g * 8 + j, 8, stride=0), :]
                    unit = unit_s[k, pl.ds(g * 8 + j, 8, stride=0), :]
                    for n in range(held):
                        word[n] = word[n] + jnp.where(which == sub + 8 * n, unit, 0)
                low = [a + (w & nibbles) for a, w in zip(low, word)]
                high = [a + ((w >> 4) & nibbles) for a, w in zip(high, word)]
                return low, high

            zero = [jnp.zeros((8, LANES), i32) for _ in range(held)]
            low, high = lax.fori_loop(0, slots // 8, group, (zero, list(zero)))
            live = z_ref[slots + 3 : slots + 4, lane_tile(k)]
            for n in range(held):
                for field in range(8):
                    part = low[n] if field % 2 == 0 else high[n]
                    value = ((part >> (8 * (field // 2))) & 255).astype(f32) * live
                    row = field * words + (n % per_tile) * 8
                    outs[n // per_tile][source, row : row + 8, lane_tile(k)] = value
        for out in outs:
            out[source, tile_cells : tile_cells + FEATURES, :] = z_ref[slots : slots + FEATURES, :]


def set_tables(log_rows, state, log_weight, log_s, ltp_s, par_s):
    genes, cells = log_rows.shape
    padded = log_s.shape[0]
    log_s[0:genes, :] = log_rows
    if padded > genes:
        log_s[genes:padded, :] = jnp.zeros((padded - genes, cells), f32)
    rest = log_s[...].T
    for part in range(PARTS):
        piece = rest.astype(bf16)
        ltp_s[part * cells : (part + 1) * cells, :] = piece
        if part + 1 < PARTS:
            rest = rest - piece.astype(f32)
    mu_row, mu_col, rr, rc, cc = state
    det = rr * cc - rc * rc
    rows = [
        mu_row,
        mu_col,
        -0.5 * (cc / det),
        rc / det,
        -0.5 * (rr / det),
        log_weight - 0.5 * jnp.log(det),
        jnp.zeros((LANES - 6, cells), f32),
    ]
    columns = jnp.concatenate(rows, axis=0).T
    for n in range(6):
        par_s[n] = jnp.broadcast_to(columns[:, n : n + 1], (cells, LANES))


def gene_hot(x_ref, source, cells, padded):
    tokens = x_ref.shape[2]
    gene = x_ref[source, cells + 2 : cells + 3, :].astype(i32)
    axis = lax.broadcasted_iota(i32, (padded, tokens), 0)
    return jnp.where(axis == gene, 1.0, 0.0).astype(bf16)


def neighbour(source, side):
    rows, cols = lax.axis_size("row"), lax.axis_size("col")
    row = lax.axis_index("row") + source - 1
    col = lax.axis_index("col") + side - 1
    inside = (row >= 0) & (row < rows) & (col >= 0) & (col < cols)
    at = jnp.clip(row, 0, rows - 1) * cols + jnp.clip(col, 0, cols - 1)
    return inside, at


def score_block(x_ref, source, side, hot, ltp_s, par_s, gl_s, sc_s, e_ref, m_ref, out_ref):
    cells = sc_s.shape[0]
    tokens = sc_s.shape[1]
    tiles = tokens // LANES
    gl_s[...] = jnp.dot(ltp_s[...], hot, preferred_element_type=f32)
    step_row = (source - 1).astype(f32) if hasattr(source, "astype") else float(source - 1)
    y0 = [x_ref[source, cells : cells + 1, lane_tile(k)] + step_row for k in range(tiles)]
    y1 = [x_ref[source, cells + 1 : cells + 2, lane_tile(k)] + float(side - 1) for k in range(tiles)]
    block = source * 3 + side

    def first(c, top):
        at = pl.multiple_of(c * 8, 8)
        p = [par_s[n, pl.ds(at, 8), :] for n in range(6)]
        out = []
        for k in range(tiles):
            d0 = y0[k] - p[0]
            d1 = y1[k] - p[1]
            logs = gl_s[pl.ds(at, 8), lane_tile(k)]
            for part in range(1, PARTS):
                logs = logs + gl_s[pl.ds(part * cells + at, 8), lane_tile(k)]
            score = logs + p[5] + (d0 * (p[2] * d0 + p[3] * d1) + p[4] * d1 * d1)
            count = x_ref[source, pl.ds(at, 8), lane_tile(k)]
            score = jnp.where(count > 0.0, score, NEVER)
            sc_s[pl.ds(at, 8), lane_tile(k)] = score
            out.append(jnp.maximum(top[k], score))
        return out

    top = lax.fori_loop(0, cells // 8, first, [jnp.full((8, LANES), NEVER, f32)] * tiles, unroll=2)
    top = [jnp.max(a, axis=0, keepdims=True) for a in top]

    def second(c, total):
        at = pl.multiple_of(c * 8, 8)
        out = []
        for k in range(tiles):
            e = x_ref[source, pl.ds(at, 8), lane_tile(k)] * jnp.exp(
                sc_s[pl.ds(at, 8), lane_tile(k)] - top[k]
            )
            e_ref[block, pl.ds(at, 8), lane_tile(k)] = e
            out.append(total[k] + e)
        return out

    total = lax.fori_loop(0, cells // 8, second, [jnp.zeros((8, LANES), f32)] * tiles, unroll=2)
    total = [jnp.sum(a, axis=0, keepdims=True) for a in total]
    both = jnp.concatenate(top + total, axis=0)
    m_ref[block] = both
    inside, at = neighbour(source, side)

    @pl.when(inside)
    def _():
        out_ref[at] = both


def first_kernel(
    w_ref, centre_ref, spread_ref, corr_ref, left_ref, mid_ref, right_ref,
    e_ref, m_ref, out_ref, state_ref,
    log_s, ltp_s, par_s, gl_s, sc_s,
):
    weights = w_ref[...]
    profile = weights / jnp.sum(weights, axis=0, keepdims=True)
    spread_row, spread_col = spread_ref[0:1, :], spread_ref[1:2, :]
    state = (
        centre_ref[0:1, :],
        centre_ref[1:2, :],
        spread_row * spread_row,
        corr_ref[0:1, :] * spread_row * spread_col,
        spread_col * spread_col,
    )
    cells = weights.shape[1]
    state_ref[...] = jnp.concatenate(list(state) + [jnp.zeros((3, cells), f32)], axis=0)
    set_tables(jnp.log(profile), state, jnp.zeros((1, cells), f32), log_s, ltp_s, par_s)
    out_ref[...] = jnp.zeros(out_ref.shape, f32)
    for side, x_ref in enumerate((left_ref, mid_ref, right_ref)):

        @pl.loop(0, 3)
        def _(source):
            hot = gene_hot(x_ref, source, cells, log_s.shape[0])
            score_block(x_ref, source, side, hot, ltp_s, par_s, gl_s, sc_s, e_ref, m_ref, out_ref)


def join_kernel(in_ref, out_ref):
    half = in_ref.shape[1] // 2
    parts = []
    for source in range(3):
        for side in range(3):
            inside, at = neighbour(source, side)
            part = in_ref[at]
            parts.append((jnp.where(inside, part[0:half], NEVER), jnp.where(inside, part[half:], 0.0)))
    top = functools.reduce(jnp.maximum, [m for m, _ in parts])
    total = sum(s * jnp.exp(m - top) for m, s in parts)
    factor = jnp.where(total > 0.0, 1.0 / total, 0.0)
    both = jnp.concatenate([top, factor], axis=0)
    for at in range(out_ref.shape[0]):
        out_ref[at] = both


def posterior_sums(x_refs, e_ref, m_ref, q_ref, hot_s, sh_s, mom_s, cnt_s, keep):
    cells, tokens = sh_s.shape
    tiles = tokens // LANES
    mom_s[...] = jnp.zeros(mom_s.shape, f32)
    cnt_s[...] = jnp.zeros(cnt_s.shape, f32)
    for side, x_ref in enumerate(x_refs):

        @pl.loop(0, 3)
        def _(source):
            block = source * 3 + side
            slot = block if keep else 0
            hot_s[slot] = gene_hot(x_ref, source, cells, cnt_s.shape[0])
            inside, at = neighbour(source, side)
            step_row = (source - 1).astype(f32)
            factor, features = [], []
            for k in range(tiles):
                m = m_ref[block, k : k + 1, :]
                f = jnp.exp(m - q_ref[at, k : k + 1, :]) * q_ref[at, tiles + k : tiles + k + 1, :]
                factor.append(jnp.where(inside, f, 0.0))
                y0 = x_ref[source, cells : cells + 1, lane_tile(k)] + step_row
                y1 = x_ref[source, cells + 1 : cells + 2, lane_tile(k)] + float(side - 1)
                features.append((y0, y1, y0 * y0, y0 * y1, y1 * y1))

            def group(c, carry):
                rows = pl.ds(pl.multiple_of(c * 16, 16), 16)
                sums = [mom_s[n, rows, :] for n in range(6)]
                for k in range(tiles):
                    p = e_ref[block, rows, lane_tile(k)] * factor[k]
                    sh_s[rows, lane_tile(k)] = p.astype(bf16)
                    sums[0] = sums[0] + p
                    for n in range(5):
                        sums[n + 1] = sums[n + 1] + p * features[k][n]
                for n in range(6):
                    mom_s[n, rows, :] = sums[n]
                return carry

            lax.fori_loop(0, cells // 16, group, 0)
            cnt_s[...] += lax.dot_general(
                hot_s[slot], sh_s[...], (((1,), (1,)), ((), ())), preferred_element_type=f32
            )


def new_cells(genes, mom_s, cnt_s, state_ref):
    weight, s0, s1, s00, s01, s11 = [jnp.sum(mom_s[n].T, axis=0, keepdims=True) for n in range(6)]
    mu_row, mu_col, rr, rc, cc = [state_ref[n : n + 1, :] for n in range(5)]
    counts = cnt_s[0:genes, :]
    profile = (counts + pseudo_count) / (
        jnp.sum(counts, axis=0, keepdims=True) + genes * pseudo_count
    )
    denominator = weight + prior_weight
    new_row = (s0 + prior_weight * mu_row) / denominator
    new_col = (s1 + prior_weight * mu_col) / denominator
    q_rr = s00 - 2.0 * new_row * s0 + weight * new_row * new_row
    q_rc = s01 - new_row * s1 - new_col * s0 + weight * new_row * new_col
    q_cc = s11 - 2.0 * new_col * s1 + weight * new_col * new_col
    state = (
        new_row,
        new_col,
        (q_rr + prior_weight * rr) / denominator,
        (q_rc + prior_weight * rc) / denominator,
        (q_cc + prior_weight * cc) / denominator,
    )
    return jnp.log(profile), state, jnp.log(weight + 1.0)


def middle_kernel(
    genes,
    left_ref, mid_ref, right_ref, e_ref, m_ref, q_ref, state_ref,
    e_out, m_out, out_ref, state_out,
    hot_s, sh_s, mom_s, cnt_s, log_s, ltp_s, par_s, gl_s, sc_s,
):
    x_refs = (left_ref, mid_ref, right_ref)
    posterior_sums(x_refs, e_ref, m_ref, q_ref, hot_s, sh_s, mom_s, cnt_s, True)
    log_rows, state, log_weight = new_cells(genes, mom_s, cnt_s, state_ref)
    cells = log_rows.shape[1]
    state_out[...] = jnp.concatenate(list(state) + [jnp.zeros((3, cells), f32)], axis=0)
    set_tables(log_rows, state, log_weight, log_s, ltp_s, par_s)
    out_ref[...] = jnp.zeros(out_ref.shape, f32)
    for side, x_ref in enumerate(x_refs):

        @pl.loop(0, 3)
        def _(source):
            hot = hot_s[source * 3 + side]
            score_block(x_ref, source, side, hot, ltp_s, par_s, gl_s, sc_s, e_out, m_out, out_ref)


def last_kernel(
    genes,
    left_ref, mid_ref, right_ref, e_ref, m_ref, q_ref, state_ref,
    profile_ref, cells_ref,
    hot_s, sh_s, mom_s, cnt_s,
):
    posterior_sums((left_ref, mid_ref, right_ref), e_ref, m_ref, q_ref, hot_s, sh_s, mom_s, cnt_s, False)
    log_rows, state, log_weight = new_cells(genes, mom_s, cnt_s, state_ref)
    profile_ref[...] = log_rows
    mu_row, mu_col, rr, rc, cc = state
    cells_ref[...] = jnp.concatenate(
        [mu_row, mu_col, 0.5 * jnp.log(rr), 0.5 * jnp.log(cc), rc / jnp.sqrt(rr * cc), log_weight],
        axis=0,
    )


def body(
    positions, genes, candidates, block_counts, profile_weights, centroids, spreads, correlation
):
    gene_total = profile_weights.shape[0]
    cells = profile_weights.shape[3]
    tokens, slots = candidates.shape[2:]
    tiles = tokens // LANES
    group = lax.axis_size("row") * lax.axis_size("col")
    padded = -(-gene_total // LANES) * LANES
    pairs = 9 * tokens * cells

    packed, = call(
        pack_kernel, "pack", [((slots + FEATURES, tokens), f32)],
        [SMEM, VMEM, VMEM, VMEM], [], tokens * slots,
        (
            block_counts.reshape(-1),
            candidates.reshape(tokens, slots),
            positions.reshape(2 * tiles, LANES),
            genes.reshape(tiles, LANES),
        ),
    )
    from_up = shifted(packed, "row", 1)
    from_down = shifted(packed, "row", -1)
    three = ((3, cells + FEATURES, tokens), f32)
    to_left, mid, to_right = call(
        functools.partial(multiple_kernel, cells), "multiple", [three] * 3, [VMEM] * 3,
        [pltpu.VMEM((tiles, slots, LANES), i32)] * 2, pairs * 40,
        (from_up, packed, from_down),
    )
    from_right = shifted(to_left, "col", -1)
    from_left = shifted(to_right, "col", 1)
    x = (from_left, mid, from_right)

    kept = ((9, cells, tokens), f32)
    tops = ((9, 2 * tiles, LANES), f32)
    chunks = ((group, 2 * tiles, LANES), f32)
    rows = ((8, cells), f32)
    table_scratch = [
        pltpu.VMEM((padded, cells), f32),
        pltpu.VMEM((PARTS * cells, padded), bf16),
        pltpu.VMEM((6, cells, LANES), f32),
        pltpu.VMEM((PARTS * cells, tokens), f32),
        pltpu.VMEM((cells, tokens), f32),
    ]

    def sum_scratch(count):
        return [
            pltpu.VMEM((count, padded, tokens), bf16),
            pltpu.VMEM((cells, tokens), bf16),
            pltpu.VMEM((6, cells, LANES), f32),
            pltpu.VMEM((padded, cells), f32),
        ]

    def exchange(parts):
        back = lax.all_to_all(parts, ("row", "col"), 0, 0)
        joined, = call(join_kernel, "join", [chunks], [VMEM], [], tokens * 100, (back,))
        return lax.all_to_all(joined, ("row", "col"), 0, 0)

    e, m, parts, state = call(
        first_kernel, "first", [kept, tops, chunks, rows], [VMEM] * 7, table_scratch, pairs * 100,
        (
            profile_weights.reshape(gene_total, cells),
            centroids.reshape(2, cells),
            spreads.reshape(2, cells),
            correlation.reshape(1, cells),
            *x,
        ),
    )
    for _ in range(ITERS - 1):
        told = exchange(parts)
        e, m, parts, state = call(
            functools.partial(middle_kernel, gene_total), "middle", [kept, tops, chunks, rows],
            [VMEM] * 7, sum_scratch(9) + table_scratch, pairs * 200,
            (*x, e, m, told, state),
        )
    told = exchange(parts)
    final_profile, final_cells = call(
        functools.partial(last_kernel, gene_total), "last",
        [((gene_total, cells), f32), ((6, cells), f32)],
        [VMEM] * 7, sum_scratch(1), pairs * 100,
        (*x, e, m, told, state),
    )
    return (final_profile.reshape(gene_total, 1, 1, cells), final_cells.reshape(6, 1, 1, cells))


def solution(mesh):
    tiles = P(("groups", "row"), "col")
    stacked = P(None, ("groups", "row"), "col", None)
    return jax.shard_map(
        body,
        mesh=mesh,
        in_specs=(
            stacked,
            P(("groups", "row"), "col", None),
            P(("groups", "row"), "col", None, None),
            P(("groups", "row"), "col", None),
            stacked,
            stacked,
            stacked,
            P(("groups", "row"), "col", None),
        ),
        out_specs=(stacked, stacked),
        check_vma=False,
    )
```

```python
import functools

import jax
import jax.numpy as jnp
from jax import lax
from jax.experimental import pallas as pl
from jax.experimental.pallas import tpu as pltpu
from jax.sharding import PartitionSpec as P

BLOCK = 256
LANES = 128
FEATURES = 8
PARTS = 3
NEVER = -1e30
UNROLL = False

pseudo_count = 0.05
prior_weight = 1.0

f32 = jnp.float32
bf16 = jnp.bfloat16
i32 = jnp.int32


def shifted(x, axis, by):
    count = lax.axis_size(axis)
    pairs = [(i, i + by) for i in range(count) if 0 <= i + by < count]
    return lax.ppermute(x, axis, pairs)


def params(mib=40):
    return pltpu.CompilerParams(vmem_limit_bytes=mib << 20)


def cost(flops, size):
    return pl.CostEstimate(flops=flops, bytes_accessed=size, transcendentals=0)


def call(kernel, name, outs, in_specs, scratch, flops, args):
    shapes = [jax.ShapeDtypeStruct(s, d) for s, d in outs]
    return pl.pallas_call(
        kernel,
        name=name,
        out_shape=shapes,
        in_specs=in_specs,
        out_specs=[pl.BlockSpec(memory_space=pltpu.VMEM)] * len(shapes),
        scratch_shapes=scratch,
        compiler_params=params(),
        cost_estimate=cost(flops, 1 << 20),
    )(*args)


VMEM = pl.BlockSpec(memory_space=pltpu.VMEM)
SMEM = pl.BlockSpec(memory_space=pltpu.SMEM)
ANY = pl.BlockSpec(memory_space=pltpu.HBM)


def lane_tile(k):
    return pl.ds(k * LANES, LANES)


def padded_to(size, unit):
    return -(-size // unit) * unit


def sources(step):
    if UNROLL:
        for source in range(3):
            step(source)
    else:
        pl.loop(0, 3)(step)


def as_float(x):
    return x.astype(f32) if hasattr(x, "astype") else float(x)


def table_rows(profile, state, log_weight):
    genes, cells = profile.shape
    mu_row, mu_col, rr, rc, cc = state
    det = rr * cc - rc * rc
    rows = [jnp.log(profile)]
    if genes % 8:
        rows.append(jnp.zeros((-genes % 8, cells), f32))
    rows += [
        mu_row,
        mu_col,
        -0.5 * (cc / det),
        rc / det,
        -0.5 * (rr / det),
        log_weight - 0.5 * jnp.log(det),
        jnp.zeros((2, cells), f32),
    ]
    return jnp.concatenate(rows, axis=0)


def state_rows(state):
    return jnp.concatenate(list(state) + [jnp.zeros((3, state[0].shape[1]), f32)], axis=0)


def pack_kernel(
    count_ref, cand_hbm, pos_hbm, gene_hbm, weight_hbm, centre_hbm, spread_hbm, corr_hbm,
    out_ref, table_ref, state_ref,
    cand_ref, pos_ref, gene_ref, weight_ref, centre_ref, spread_ref, corr_ref, sems,
):
    pairs = (
        (cand_hbm, cand_ref), (pos_hbm, pos_ref), (gene_hbm, gene_ref), (weight_hbm, weight_ref),
        (centre_hbm, centre_ref), (spread_hbm, spread_ref), (corr_hbm, corr_ref),
    )
    copies = [pltpu.make_async_copy(a, b, sems.at[n]) for n, (a, b) in enumerate(pairs)]
    for copy in copies:
        copy.start()
    for copy in copies[:3]:
        copy.wait()
    tokens, slots = cand_ref.shape
    tiles = tokens // LANES
    out_ref[0:slots, :] = cand_ref[...].astype(f32).T
    lane = lax.broadcasted_iota(i32, (1, LANES), 1)
    for k in range(tiles):
        start = k * LANES
        live = (start % BLOCK + lane) < count_ref[start // BLOCK]
        rows = [
            pos_ref[k : k + 1, :],
            pos_ref[tiles + k : tiles + k + 1, :],
            gene_ref[k : k + 1, :].astype(f32),
            live.astype(f32),
            jnp.zeros((FEATURES - 4, LANES), f32),
        ]
        out_ref[slots : slots + FEATURES, lane_tile(k)] = jnp.concatenate(rows, axis=0)
    for copy in copies[3:]:
        copy.wait()
    weights = weight_ref[...]
    spread_row, spread_col = spread_ref[0:1, :], spread_ref[1:2, :]
    state = (
        centre_ref[0:1, :],
        centre_ref[1:2, :],
        spread_row * spread_row,
        corr_ref[0:1, :] * spread_row * spread_col,
        spread_col * spread_col,
    )
    state_ref[...] = state_rows(state)
    profile = weights / jnp.sum(weights, axis=0, keepdims=True)
    table_ref[...] = table_rows(profile, state, jnp.zeros_like(spread_row))


def count_source(source, z_ref, cells, outs, word_s, unit_s):
    rows, tokens = z_ref.shape
    slots = rows - FEATURES
    words = cells // 8
    shift = cells.bit_length() - 1
    word_shift = words.bit_length() - 1
    held = 3 * words // 8
    per_tile = words // 8
    sub = lax.broadcasted_iota(i32, (8, LANES), 0)
    nibbles = jnp.full((8, LANES), 0x0F0F0F0F, i32)
    for k in range(tokens // LANES):
        local = z_ref[0:slots, lane_tile(k)].astype(i32) - (2 - source) * 3 * cells
        word_s[k] = (local >> shift) * words + (local & (words - 1))
        unit_s[k] = 1 << (((local & (cells - 1)) >> word_shift) * 4)

    def some(k, start, amount, carry):
        low, high = carry
        word = [jnp.zeros((8, LANES), i32) for _ in range(held)]
        for j in range(amount):
            which = word_s[k, pl.ds(start + j, 8, stride=0), :]
            unit = unit_s[k, pl.ds(start + j, 8, stride=0), :]
            for n in range(held):
                word[n] = word[n] + jnp.where(which == sub + 8 * n, unit, 0)
        low = [a + (w & nibbles) for a, w in zip(low, word)]
        high = [a + ((w >> 4) & nibbles) for a, w in zip(high, word)]
        return low, high

    for k in range(tokens // LANES):
        zero = [jnp.zeros((8, LANES), i32) for _ in range(held)]
        whole = slots // 15
        carry = lax.fori_loop(
            0, whole, lambda g, carry: some(k, g * 15, 15, carry), (zero, list(zero))
        )
        if slots % 15:
            carry = some(k, whole * 15, slots % 15, carry)
        low, high = carry
        live = z_ref[slots + 3 : slots + 4, lane_tile(k)]
        for n in range(held):
            for field in range(8):
                part = low[n] if field % 2 == 0 else high[n]
                value = ((part >> (8 * (field // 2))) & 255).astype(f32) * live
                row = field * words + (n % per_tile) * 8
                outs[n // per_tile][row : row + 8, lane_tile(k)] = value
    for out in outs:
        out[cells : cells + FEATURES, :] = z_ref[slots : slots + FEATURES, :]


def own_counts_kernel(cells, own_ref, left_ref, mid_ref, right_ref, word_s, unit_s):
    count_source(1, own_ref, cells, (left_ref, mid_ref, right_ref), word_s, unit_s)


def counts_kernel(
    cells, up_ref, down_ref, own_left, own_mid, own_right, ltp_hbm,
    left_ref, mid_ref, right_ref, word_s, unit_s,
):
    outs = (left_ref, mid_ref, right_ref)
    for out, own in zip(outs, (own_left, own_mid, own_right)):
        out[1] = own[...]
    for source, z_ref in ((0, up_ref), (2, down_ref)):
        count_source(source, z_ref, cells, [out.at[source] for out in outs], word_s, unit_s)


def load_table(table_ref, ltp_s, par_s):
    cells = table_ref.shape[1]
    padded = ltp_s.shape[1]
    genes = table_ref.shape[0] - 8
    logs = [table_ref[0:genes, :]]
    if padded > genes:
        logs.append(jnp.zeros((padded - genes, cells), f32))
    rest = jnp.concatenate(logs, axis=0).T
    for part in range(PARTS):
        piece = rest.astype(bf16)
        ltp_s[part * cells : (part + 1) * cells, :] = piece
        if part + 1 < PARTS:
            rest = rest - piece.astype(f32)
    rows = [table_ref[genes : genes + 8, :], jnp.zeros((LANES - 8, cells), f32)]
    columns = jnp.concatenate(rows, axis=0).T
    for n in range(6):
        par_s[n] = jnp.broadcast_to(columns[:, n : n + 1], (cells, LANES))


def tables_kernel(left_ref, own_ref, right_ref, ltp_ref, par_ref):
    for side, table in enumerate((left_ref, own_ref, right_ref)):
        load_table(table, ltp_ref.at[side], par_ref.at[side])


def gene_hot(x_ref, source, cells, padded):
    tokens = x_ref.shape[2]
    gene = x_ref[source, cells + 2 : cells + 3, :].astype(i32)
    axis = lax.broadcasted_iota(i32, (padded, tokens), 0)
    return jnp.where(axis == gene, 1.0, 0.0).astype(bf16)


def features(x_ref, source, cells, row_step, col_step):
    y0 = x_ref[source, cells : cells + 1, :] + row_step
    y1 = x_ref[source, cells + 1 : cells + 2, :] + col_step
    return y0, y1


def score_rows(at, y0, y1, gl_s, par_s, cells):
    tiles = y0.shape[1] // LANES
    p = [jnp.concatenate([par_s[n, at : at + 8, :]] * tiles, axis=1) for n in range(6)]
    d0 = y0 - p[0]
    d1 = y1 - p[1]
    logs = gl_s[at : at + 8, :]
    for part in range(1, PARTS):
        logs = logs + gl_s[part * cells + at : part * cells + at + 8, :]
    return logs + p[5] + (d0 * (p[2] * d0 + p[3] * d1) + p[4] * d1 * d1)


def row_of(ref, index, first, tiles):
    return jnp.concatenate([ref[index + (pl.ds(first + k, 1), slice(None))] for k in range(tiles)], axis=1)


def to_tiles(row):
    return jnp.concatenate([row[:, k * LANES : (k + 1) * LANES] for k in range(row.shape[1] // LANES)], axis=0)


def spread_rows(part_s, out_ref):
    rows = out_ref.shape[0]
    half = part_s.shape[-2] // 2
    shape = out_ref.shape[2:]
    level = lax.broadcasted_iota(i32, shape, len(shape) - 2)
    nothing = jnp.where(level < half, NEVER, 0.0)
    row = lax.axis_index("row")

    @pl.loop(0, rows)
    def _(at):
        for slot in range(3):
            source = at - row + slot
            inside = (source >= 0) & (source < 3)
            out_ref[at, slot] = jnp.where(inside, part_s[jnp.clip(source, 0, 2)], nothing)


def joined(parts):
    half = parts[0].shape[-2] // 2
    tops = [p[..., 0:half, :] for p in parts]
    top = functools.reduce(jnp.maximum, tops)
    total = sum(p[..., half:, :] * jnp.exp(m - top) for p, m in zip(parts, tops))
    return top, total


def gather_rows(in_ref):
    rows = in_ref.shape[0]
    row = lax.axis_index("row")
    shape = in_ref.shape[1:]
    half = shape[-2] // 2
    level = lax.broadcasted_iota(i32, shape, len(shape) - 2)
    nothing = jnp.where(level < half, NEVER, 0.0)
    parts = []
    for step in range(-2, 3):
        inside = (row + step >= 0) & (row + step < rows)
        parts.append(jnp.where(inside, in_ref[jnp.clip(row + step, 0, rows - 1)], nothing))
    return joined(parts)


def told(top, total):
    return jnp.concatenate([top, jnp.where(total > 0.0, 1.0 / total, 0.0)], axis=-2)


def row_parts_kernel(
    left_ref, mid_ref, right_ref, ltp_s, par_s, out_ref, part_s, gl_s, sc_s
):
    x_refs = (left_ref, mid_ref, right_ref)
    cells, tokens = sc_s.shape[1:]

    def step(source):
        hot = gene_hot(mid_ref, source, cells, ltp_s.shape[2])
        for side in range(3):
            gl_s[side] = jnp.dot(ltp_s[side], hot, preferred_element_type=f32)
        top = jnp.full((8, tokens), NEVER, f32)
        for side in range(3):
            y0, y1 = features(mid_ref, source, cells, as_float(source) - 1.0, 1.0 - side)
            for at in range(0, cells, 8):
                score = score_rows(at, y0, y1, gl_s.at[side], par_s.at[side], cells)
                score = jnp.where(x_refs[side][source, at : at + 8, :] > 0.0, score, NEVER)
                sc_s[side, at : at + 8, :] = score
                top = jnp.maximum(top, score)
        top = jnp.max(top, axis=0, keepdims=True)
        total = jnp.zeros((8, tokens), f32)
        for side in range(3):
            for at in range(0, cells, 8):
                count = x_refs[side][source, at : at + 8, :]
                total = total + count * jnp.exp(sc_s[side, at : at + 8, :] - top)
        total = jnp.sum(total, axis=0, keepdims=True)
        part_s[source] = jnp.concatenate([to_tiles(top), to_tiles(total)], axis=0)

    sources(step)
    spread_rows(part_s, out_ref)


def row_join_kernel(in_ref, out_ref):
    out_ref[...] = told(*gather_rows(in_ref))


def part_join_kernel(in_ref, out_ref):
    out_ref[...] = jnp.concatenate(gather_rows(in_ref), axis=-2)


def add_moments(p, y0, y1, sums):
    def fold(x):
        parts = [x[:, k * LANES : (k + 1) * LANES] for k in range(x.shape[1] // LANES)]
        return functools.reduce(jnp.add, parts)

    weights = (None, y0, y1, y0 * y0, y0 * y1, y1 * y1)
    return [s + fold(p if w is None else p * w) for s, w in zip(sums, weights)]


def add_counts(hot, sh_s, cnt_s):
    cnt_s[...] += lax.dot_general(hot, sh_s[...], (((1,), (1,)), ((), ())), preferred_element_type=f32)


def new_cells(genes, mom_s, cnt_s, state_ref):
    weight, s0, s1, s00, s01, s11 = [jnp.sum(mom_s[n].T, axis=0, keepdims=True) for n in range(6)]
    mu_row, mu_col, rr, rc, cc = [state_ref[n : n + 1, :] for n in range(5)]
    counts = cnt_s[0:genes, :]
    profile = (counts + pseudo_count) / (
        jnp.sum(counts, axis=0, keepdims=True) + genes * pseudo_count
    )
    denominator = weight + prior_weight
    new_row = (s0 + prior_weight * mu_row) / denominator
    new_col = (s1 + prior_weight * mu_col) / denominator
    q_rr = s00 - 2.0 * new_row * s0 + weight * new_row * new_row
    q_rc = s01 - new_row * s1 - new_col * s0 + weight * new_row * new_col
    q_cc = s11 - 2.0 * new_col * s1 + weight * new_col * new_col
    state = (
        new_row,
        new_col,
        (q_rr + prior_weight * rr) / denominator,
        (q_rc + prior_weight * rc) / denominator,
        (q_cc + prior_weight * cc) / denominator,
    )
    return profile, state, jnp.log(weight + 1.0)


def middle_kernel(
    genes,
    left_ref, mid_ref, right_ref, ltp_ref, par_ref, state_ref, told_ref,
    e_ref, m_ref, out_ref, state_out,
    hot_s, sh_s, mom_s, cnt_s, ltp_s, par_s, gl_s, sc_s, table_s, part_s,
):
    x_refs = (left_ref, mid_ref, right_ref)
    cells, tokens = sc_s.shape[1:]
    tiles = tokens // LANES
    padded = cnt_s.shape[0]
    cols = told_ref.shape[0]
    col = lax.axis_index("col")
    mom_s[...] = jnp.zeros(mom_s.shape, f32)
    cnt_s[...] = jnp.zeros(cnt_s.shape, f32)

    def posterior(source):
        for side, x_ref in enumerate(x_refs):
            hot_s[source, side] = gene_hot(x_ref, source, cells, padded)
            gl_s[side] = jnp.dot(ltp_ref[1], hot_s[source, side], preferred_element_type=f32)
        for side, x_ref in enumerate(x_refs):
            at_col = jnp.clip(col + side - 1, 0, cols - 1)
            top = row_of(told_ref, (at_col, source), 0, tiles)
            factor = row_of(told_ref, (at_col, source), tiles, tiles)
            y0, y1 = features(x_ref, source, cells, as_float(source) - 1.0, side - 1.0)
            for at in range(0, cells, 16):
                halves = []
                for a in (at, at + 8):
                    score = score_rows(a, y0, y1, gl_s.at[side], par_ref.at[1], cells)
                    count = x_ref[source, a : a + 8, :]
                    p = count * jnp.exp(jnp.minimum(score - top, 0.0)) * factor
                    sums = [mom_s[n, a : a + 8, :] for n in range(6)]
                    sums = add_moments(p, y0, y1, sums)
                    for n in range(6):
                        mom_s[n, a : a + 8, :] = sums[n]
                    halves.append(p)
                sh_s[side, at : at + 16, :] = jnp.concatenate(halves, axis=0).astype(bf16)
            add_counts(hot_s[source, side], sh_s.at[side], cnt_s)

    sources(posterior)
    profile, state, log_weight = new_cells(genes, mom_s, cnt_s, state_ref)
    state_out[...] = state_rows(state)
    table_s[...] = table_rows(profile, state, log_weight)
    load_table(table_s, ltp_s, par_s)

    def score(source):
        for side in range(3):
            gl_s[side] = jnp.dot(ltp_s[...], hot_s[source, side], preferred_element_type=f32)
        for side, x_ref in enumerate(x_refs):
            y0, y1 = features(x_ref, source, cells, as_float(source) - 1.0, side - 1.0)
            top = jnp.full((8, tokens), NEVER, f32)
            for at in range(0, cells, 8):
                value = score_rows(at, y0, y1, gl_s.at[side], par_s, cells)
                value = jnp.where(x_ref[source, at : at + 8, :] > 0.0, value, NEVER)
                sc_s[side, at : at + 8, :] = value
                top = jnp.maximum(top, value)
            top = jnp.max(top, axis=0, keepdims=True)
            total = jnp.zeros((8, tokens), f32)
            for at in range(0, cells, 8):
                e = x_ref[source, at : at + 8, :] * jnp.exp(sc_s[side, at : at + 8, :] - top)
                e_ref[source, side, at : at + 8, :] = e
                total = total + e
            total = jnp.sum(total, axis=0, keepdims=True)
            part_s[source, side] = jnp.concatenate([to_tiles(top), to_tiles(total)], axis=0)

    sources(score)
    m_ref[...] = part_s[...]
    spread_rows(part_s, out_ref)


def last_kernel(
    genes,
    left_ref, mid_ref, right_ref, e_ref, m_ref, told_ref, state_ref,
    profile_ref, cells_ref,
    sh_s, mom_s, cnt_s,
):
    x_refs = (left_ref, mid_ref, right_ref)
    cells, tokens = sh_s.shape[1:]
    tiles = tokens // LANES
    cols = told_ref.shape[0]
    col = lax.axis_index("col")
    mom_s[...] = jnp.zeros(mom_s.shape, f32)
    cnt_s[...] = jnp.zeros(cnt_s.shape, f32)
    shape = m_ref.shape[2:]
    nothing = jnp.where(lax.broadcasted_iota(i32, shape, 0) < shape[0] // 2, NEVER, 0.0)

    def posterior(source):
        for side, x_ref in enumerate(x_refs):
            parts = []
            for step in range(-1, 2):
                owner = col + side - 1 + step
                inside = (owner >= 0) & (owner < cols)
                part = told_ref[jnp.clip(owner, 0, cols - 1), source, 1 - step]
                parts.append(jnp.where(inside, part, nothing))
            top, total = joined(parts)
            scale = jnp.exp(m_ref[source, side][0:tiles] - top)
            scale = jnp.where(total > 0.0, scale / total, 0.0)
            factor = jnp.concatenate([scale[k : k + 1, :] for k in range(tiles)], axis=1)
            y0, y1 = features(x_ref, source, cells, as_float(source) - 1.0, side - 1.0)
            for at in range(0, cells, 16):
                halves = []
                for a in (at, at + 8):
                    p = e_ref[source, side, a : a + 8, :] * factor
                    sums = [mom_s[n, a : a + 8, :] for n in range(6)]
                    sums = add_moments(p, y0, y1, sums)
                    for n in range(6):
                        mom_s[n, a : a + 8, :] = sums[n]
                    halves.append(p)
                sh_s[side, at : at + 16, :] = jnp.concatenate(halves, axis=0).astype(bf16)
            add_counts(gene_hot(x_ref, source, cells, cnt_s.shape[0]), sh_s.at[side], cnt_s)

    sources(posterior)
    profile, state, log_weight = new_cells(genes, mom_s, cnt_s, state_ref)
    profile_ref[...] = jnp.log(profile)
    mu_row, mu_col, rr, rc, cc = state
    final = (mu_row, mu_col, 0.5 * jnp.log(rr), 0.5 * jnp.log(cc), rc / jnp.sqrt(rr * cc), log_weight)
    for n, row in enumerate(final):
        cells_ref[n] = row


def body(
    positions, genes, candidates, block_counts, profile_weights, centroids, spreads, correlation
):
    gene_total = profile_weights.shape[0]
    cells = profile_weights.shape[3]
    tokens, slots = candidates.shape[2:]
    tiles = tokens // LANES
    rows = lax.axis_size("row")
    padded = padded_to(gene_total, LANES)
    pairs = 9 * tokens * cells
    table = ((padded_to(gene_total, 8) + 8, cells), f32)
    state = ((8, cells), f32)
    vmem = pltpu.VMEM

    packed, table_own, state_own = call(
        pack_kernel, "pack", [((slots + FEATURES, tokens), f32), table, state],
        [SMEM] + [ANY] * 7,
        [
            vmem((tokens, slots), i32),
            vmem((2 * tiles, LANES), f32),
            vmem((tiles, LANES), i32),
            vmem((gene_total, cells), f32),
            vmem((2, cells), f32),
            vmem((2, cells), f32),
            vmem((1, cells), f32),
            pltpu.SemaphoreType.DMA((7,)),
        ],
        tokens * slots,
        (
            block_counts.reshape(-1),
            candidates.reshape(tokens, slots),
            positions.reshape(2 * tiles, LANES),
            genes.reshape(tiles, LANES),
            profile_weights.reshape(gene_total, cells),
            centroids.reshape(2, cells),
            spreads.reshape(2, cells),
            correlation.reshape(1, cells),
        ),
    )
    from_up = shifted(packed, "row", 1)
    from_down = shifted(packed, "row", -1)
    table_left = shifted(table_own, "col", 1)
    table_right = shifted(table_own, "col", -1)
    ltp, par = call(
        tables_kernel, "tables",
        [((3, PARTS * cells, padded), bf16), ((3, 6, cells, LANES), f32)], [VMEM] * 3, [],
        tokens * slots, (table_left, table_own, table_right),
    )
    one = ((cells + FEATURES, tokens), f32)
    three = ((3, cells + FEATURES, tokens), f32)
    count_scratch = [vmem((tiles, slots, LANES), i32)] * 2
    own = call(
        functools.partial(own_counts_kernel, cells), "own_counts", [one] * 3, [VMEM],
        count_scratch, pairs * 40, (packed,),
    )
    to_left, mid, to_right = call(
        functools.partial(counts_kernel, cells), "counts", [three] * 3, [VMEM] * 5 + [ANY],
        count_scratch, pairs * 80, (from_up, from_down, *own, ltp),
    )
    from_right = shifted(to_left, "col", -1)
    from_left = shifted(to_right, "col", 1)

    chunk = (2 * tiles, LANES)
    parts, = call(
        row_parts_kernel, "row_parts", [((rows, 3) + chunk, f32)], [VMEM] * 5,
        [
            vmem((3,) + chunk, f32),
            vmem((3, PARTS * cells, tokens), f32),
            vmem((3, cells, tokens), f32),
        ],
        pairs * 100,
        (to_left, mid, to_right, ltp, par),
    )
    back = lax.all_to_all(parts, "row", 0, 0)
    sums, = call(row_join_kernel, "row_join", [((3,) + chunk, f32)], [VMEM], [], tokens * 100, (back,))
    told_all = lax.all_gather(sums, "col", axis=0)

    x = (from_left, mid, from_right)
    sum_scratch = [
        vmem((3, cells, tokens), bf16),
        vmem((6, cells, LANES), f32),
        vmem((padded, cells), f32),
    ]
    e, m, parts, state_own = call(
        functools.partial(middle_kernel, gene_total), "middle",
        [((3, 3, cells, tokens), f32), ((3, 3) + chunk, f32), ((rows, 3, 3) + chunk, f32), state],
        [VMEM] * 7,
        [vmem((3, 3, padded, tokens), bf16)] + sum_scratch + [
            vmem((PARTS * cells, padded), bf16),
            vmem((6, cells, LANES), f32),
            vmem((3, PARTS * cells, tokens), f32),
            vmem((3, cells, tokens), f32),
            vmem(*table),
            vmem((3, 3) + chunk, f32),
        ],
        pairs * 200,
        (*x, ltp, par, state_own, told_all),
    )
    back = lax.all_to_all(parts, "row", 0, 0)
    sums, = call(part_join_kernel, "part_join", [((3, 3) + chunk, f32)], [VMEM], [], tokens * 100, (back,))
    told_all = lax.all_gather(sums, "col", axis=0)
    final_profile, final_cells = call(
        functools.partial(last_kernel, gene_total), "last",
        [((gene_total, cells), f32), ((6, 1, cells), f32)],
        [VMEM] * 7, sum_scratch, pairs * 100,
        (*x, e, m, told_all, state_own),
    )
    return (final_profile.reshape(gene_total, 1, 1, cells), final_cells.reshape(6, 1, 1, cells))


def solution(mesh):
    tiles = P(("groups", "row"), "col")
    stacked = P(None, ("groups", "row"), "col", None)
    return jax.shard_map(
        body,
        mesh=mesh,
        in_specs=(
            stacked,
            P(("groups", "row"), "col", None),
            P(("groups", "row"), "col", None, None),
            P(("groups", "row"), "col", None),
            stacked,
            stacked,
            stacked,
            P(("groups", "row"), "col", None),
        ),
        out_specs=(stacked, stacked),
        check_vma=False,
    )
```

```python
import functools

import jax
import jax.numpy as jnp
from jax import lax
from jax.experimental import pallas as pl
from jax.experimental.pallas import tpu as pltpu
from jax.sharding import PartitionSpec as P

BLOCK = 256
LANES = 128
FEATURES = 8
PARTS = 2
NEVER = -1e30
UNROLL = True

pseudo_count = 0.05
prior_weight = 1.0

f32 = jnp.float32
bf16 = jnp.bfloat16
i32 = jnp.int32


def shifted(x, axis, by):
    count = lax.axis_size(axis)
    pairs = [(i, i + by) for i in range(count) if 0 <= i + by < count]
    return lax.ppermute(x, axis, pairs)


def params(mib=40):
    return pltpu.CompilerParams(vmem_limit_bytes=mib << 20)


def cost(flops, size):
    return pl.CostEstimate(flops=flops, bytes_accessed=size, transcendentals=0)


def call(kernel, name, outs, in_specs, scratch, flops, args):
    shapes = [jax.ShapeDtypeStruct(s, d) for s, d in outs]
    return pl.pallas_call(
        kernel,
        name=name,
        out_shape=shapes,
        in_specs=in_specs,
        out_specs=[pl.BlockSpec(memory_space=pltpu.VMEM)] * len(shapes),
        scratch_shapes=scratch,
        compiler_params=params(),
        cost_estimate=cost(flops, 1 << 20),
    )(*args)


VMEM = pl.BlockSpec(memory_space=pltpu.VMEM)
SMEM = pl.BlockSpec(memory_space=pltpu.SMEM)
ANY = pl.BlockSpec(memory_space=pltpu.HBM)


def lane_tile(k):
    return pl.ds(k * LANES, LANES)


def padded_to(size, unit):
    return -(-size // unit) * unit


def sources(step):
    if UNROLL:
        for source in range(3):
            step(source)
    else:
        pl.loop(0, 3)(step)


def as_float(x):
    return x.astype(f32) if hasattr(x, "astype") else float(x)


def table_rows(profile, state, log_weight):
    genes, cells = profile.shape
    mu_row, mu_col, rr, rc, cc = state
    det = rr * cc - rc * rc
    rows = [jnp.log(profile)]
    if genes % 8:
        rows.append(jnp.zeros((-genes % 8, cells), f32))
    rows += [
        mu_row,
        mu_col,
        -0.5 * (cc / det),
        rc / det,
        -0.5 * (rr / det),
        log_weight - 0.5 * jnp.log(det),
        jnp.zeros((2, cells), f32),
    ]
    return jnp.concatenate(rows, axis=0)


def state_rows(state):
    return jnp.concatenate(list(state) + [jnp.zeros((3, state[0].shape[1]), f32)], axis=0)


def pack_kernel(
    count_hbm, cand_hbm, pos_hbm, gene_hbm, weight_hbm, centre_hbm, spread_hbm, corr_hbm,
    out_ref, table_ref, state_ref,
    count_ref, cand_ref, pos_ref, gene_ref, weight_ref, centre_ref, spread_ref, corr_ref, sems,
):
    pairs = (
        (count_hbm, count_ref), (cand_hbm, cand_ref), (pos_hbm, pos_ref), (gene_hbm, gene_ref), (weight_hbm, weight_ref),
        (centre_hbm, centre_ref), (spread_hbm, spread_ref), (corr_hbm, corr_ref),
    )
    copies = [pltpu.make_async_copy(a, b, sems.at[n]) for n, (a, b) in enumerate(pairs)]
    for copy in copies:
        copy.start()
    for copy in copies[:4]:
        copy.wait()
    tokens, slots = cand_ref.shape
    tiles = tokens // LANES
    out_ref[0:slots, :] = cand_ref[...].astype(f32).T
    lane = lax.broadcasted_iota(i32, (1, LANES), 1)
    for k in range(tiles):
        start = k * LANES
        live = (start % BLOCK + lane) < count_ref[:, start // BLOCK : start // BLOCK + 1]
        rows = [
            pos_ref[k : k + 1, :],
            pos_ref[tiles + k : tiles + k + 1, :],
            gene_ref[k : k + 1, :].astype(f32),
            live.astype(f32),
            jnp.zeros((FEATURES - 4, LANES), f32),
        ]
        out_ref[slots : slots + FEATURES, lane_tile(k)] = jnp.concatenate(rows, axis=0)
    for copy in copies[4:]:
        copy.wait()
    weights = weight_ref[...]
    spread_row, spread_col = spread_ref[0:1, :], spread_ref[1:2, :]
    state = (
        centre_ref[0:1, :],
        centre_ref[1:2, :],
        spread_row * spread_row,
        corr_ref[0:1, :] * spread_row * spread_col,
        spread_col * spread_col,
    )
    state_ref[...] = state_rows(state)
    profile = weights / jnp.sum(weights, axis=0, keepdims=True)
    table_ref[...] = table_rows(profile, state, jnp.zeros_like(spread_row))


def count_source(source, z_ref, cells, outs, word_s, unit_s):
    rows, tokens = z_ref.shape
    slots = rows - FEATURES
    words = cells // 8
    shift = cells.bit_length() - 1
    word_shift = words.bit_length() - 1
    held = 3 * words // 8
    per_tile = words // 8
    sub = lax.broadcasted_iota(i32, (8, LANES), 0)
    nibbles = jnp.full((8, LANES), 0x0F0F0F0F, i32)
    for k in range(tokens // LANES):
        local = z_ref[0:slots, lane_tile(k)].astype(i32) - (2 - source) * 3 * cells
        word_s[k, 0:slots, :] = (local >> shift) * words + (local & (words - 1))
        unit_s[k, 0:slots, :] = 1 << (((local & (cells - 1)) >> word_shift) * 4)

    def some(k, start, amount, carry):
        low, high = carry
        word = [jnp.zeros((8, LANES), i32) for _ in range(held)]
        for j in range(amount):
            which = word_s[k, pl.ds(start + j, 8, stride=0), :]
            unit = unit_s[k, pl.ds(start + j, 8, stride=0), :]
            for n in range(held):
                word[n] = word[n] + jnp.where(which == sub + 8 * n, unit, 0)
        low = [a + (w & nibbles) for a, w in zip(low, word)]
        high = [a + ((w >> 4) & nibbles) for a, w in zip(high, word)]
        return low, high

    for k in range(tokens // LANES):
        zero = [jnp.zeros((8, LANES), i32) for _ in range(held)]
        whole = slots // 15
        carry = lax.fori_loop(
            0, whole, lambda g, carry: some(k, g * 15, 15, carry), (zero, list(zero))
        )
        if slots % 15:
            carry = some(k, whole * 15, slots % 15, carry)
        low, high = carry
        live = z_ref[slots + 3 : slots + 4, lane_tile(k)]
        for n in range(held):
            for field in range(8):
                part = low[n] if field % 2 == 0 else high[n]
                value = ((part >> (8 * (field // 2))) & 255).astype(f32) * live
                row = field * words + (n % per_tile) * 8
                outs[n // per_tile][row : row + 8, lane_tile(k)] = value
    for out in outs:
        out[cells : cells + FEATURES, :] = z_ref[slots : slots + FEATURES, :]


def own_counts_kernel(cells, own_ref, left_ref, mid_ref, right_ref, word_s, unit_s):
    count_source(1, own_ref, cells, (left_ref, mid_ref, right_ref), word_s, unit_s)


def counts_kernel(
    cells, up_ref, down_ref, own_left, own_mid, own_right, ltp_hbm,
    left_ref, mid_ref, right_ref, word_s, unit_s,
):
    outs = (left_ref, mid_ref, right_ref)
    for out, own in zip(outs, (own_left, own_mid, own_right)):
        out[1] = own[...]
    for source, z_ref in ((0, up_ref), (2, down_ref)):
        count_source(source, z_ref, cells, [out.at[source] for out in outs], word_s, unit_s)


def load_table(table_ref, ltp_s, par_s):
    cells = table_ref.shape[1]
    padded = ltp_s.shape[1]
    genes = table_ref.shape[0] - 8
    logs = [table_ref[0:genes, :]]
    if padded > genes:
        logs.append(jnp.zeros((padded - genes, cells), f32))
    rest = jnp.concatenate(logs, axis=0).T
    for part in range(PARTS):
        piece = rest.astype(bf16)
        ltp_s[part * cells : (part + 1) * cells, :] = piece
        if part + 1 < PARTS:
            rest = rest - piece.astype(f32)
    rows = [table_ref[genes : genes + 8, :], jnp.zeros((LANES - 8, cells), f32)]
    columns = jnp.concatenate(rows, axis=0).T
    for n in range(6):
        par_s[n] = jnp.broadcast_to(columns[:, n : n + 1], (cells, LANES))


def tables_kernel(left_ref, own_ref, right_ref, ltp_ref, par_ref):
    for side, table in enumerate((left_ref, own_ref, right_ref)):
        load_table(table, ltp_ref.at[side], par_ref.at[side])


def gene_hot(x_ref, source, cells, padded):
    tokens = x_ref.shape[2]
    gene = x_ref[source, cells + 2 : cells + 3, :].astype(i32).astype(jnp.int16)
    axis = lax.broadcasted_iota(jnp.int16, (padded, tokens), 0)
    return jnp.where(axis == gene, jnp.ones((), bf16), jnp.zeros((), bf16))


def features(x_ref, source, cells, row_step, col_step):
    y0 = x_ref[source, cells : cells + 1, :] + row_step
    y1 = x_ref[source, cells + 1 : cells + 2, :] + col_step
    return y0, y1


def score_rows(at, y0, y1, gl_s, par_s, cells):
    tiles = y0.shape[1] // LANES
    p = [jnp.concatenate([par_s[n, at : at + 8, :]] * tiles, axis=1) for n in range(6)]
    d0 = y0 - p[0]
    d1 = y1 - p[1]
    logs = gl_s[at : at + 8, :]
    for part in range(1, PARTS):
        logs = logs + gl_s[part * cells + at : part * cells + at + 8, :]
    return logs + p[5] + (d0 * (p[2] * d0 + p[3] * d1) + p[4] * d1 * d1)


def row_of(ref, index, first, tiles):
    return jnp.concatenate([ref[index + (pl.ds(first + k, 1), slice(None))] for k in range(tiles)], axis=1)


def to_tiles(row):
    return jnp.concatenate([row[:, k * LANES : (k + 1) * LANES] for k in range(row.shape[1] // LANES)], axis=0)


def spread_rows(part_s, out_ref):
    rows = out_ref.shape[0]
    half = part_s.shape[-2] // 2
    shape = out_ref.shape[2:]
    level = lax.broadcasted_iota(i32, shape, len(shape) - 2)
    nothing = jnp.where(level < half, NEVER, 0.0)
    row = lax.axis_index("row")

    @pl.loop(0, rows)
    def _(at):
        for slot in range(3):
            source = at - row + slot
            inside = (source >= 0) & (source < 3)
            out_ref[at, slot] = jnp.where(inside, part_s[jnp.clip(source, 0, 2)], nothing)


def joined(parts):
    half = parts[0].shape[-2] // 2
    tops = [p[..., 0:half, :] for p in parts]
    top = functools.reduce(jnp.maximum, tops)
    total = sum(p[..., half:, :] * jnp.exp(m - top) for p, m in zip(parts, tops))
    return top, total


def gather_rows(in_ref):
    rows = in_ref.shape[0]
    row = lax.axis_index("row")
    shape = in_ref.shape[1:]
    half = shape[-2] // 2
    level = lax.broadcasted_iota(i32, shape, len(shape) - 2)
    nothing = jnp.where(level < half, NEVER, 0.0)
    parts = []
    for step in range(-2, 3):
        inside = (row + step >= 0) & (row + step < rows)
        parts.append(jnp.where(inside, in_ref[jnp.clip(row + step, 0, rows - 1)], nothing))
    return joined(parts)


def told(top, total):
    return jnp.concatenate([top, jnp.where(total > 0.0, 1.0 / total, 0.0)], axis=-2)


def row_parts_kernel(
    left_ref, mid_ref, right_ref, ltp_s, par_s, out_ref, part_s, gl_s, sc_s
):
    x_refs = (left_ref, mid_ref, right_ref)
    cells, tokens = sc_s.shape[1:]

    def step(source):
        hot = gene_hot(mid_ref, source, cells, ltp_s.shape[2])
        for side in range(3):
            gl_s[side] = jnp.dot(ltp_s[side], hot, preferred_element_type=f32)
        top = jnp.full((8, tokens), NEVER, f32)
        for side in range(3):
            y0, y1 = features(mid_ref, source, cells, as_float(source) - 1.0, 1.0 - side)
            for at in range(0, cells, 8):
                score = score_rows(at, y0, y1, gl_s.at[side], par_s.at[side], cells)
                score = jnp.where(x_refs[side][source, at : at + 8, :] > 0.0, score, NEVER)
                sc_s[side, at : at + 8, :] = score
                top = jnp.maximum(top, score)
        top = jnp.max(top, axis=0, keepdims=True)
        total = jnp.zeros((8, tokens), f32)
        for side in range(3):
            for at in range(0, cells, 8):
                count = x_refs[side][source, at : at + 8, :]
                total = total + count * jnp.exp(sc_s[side, at : at + 8, :] - top)
        total = jnp.sum(total, axis=0, keepdims=True)
        part_s[source] = jnp.concatenate([to_tiles(top), to_tiles(total)], axis=0)

    sources(step)
    spread_rows(part_s, out_ref)


def row_join_kernel(in_ref, out_ref):
    out_ref[...] = told(*gather_rows(in_ref))


def part_join_kernel(in_ref, out_ref):
    out_ref[...] = jnp.concatenate(gather_rows(in_ref), axis=-2)


def add_moments(p, y0, y1, sums):
    def fold(x):
        parts = [x[:, k * LANES : (k + 1) * LANES] for k in range(x.shape[1] // LANES)]
        return functools.reduce(jnp.add, parts)

    weights = (None, y0, y1, y0 * y0, y0 * y1, y1 * y1)
    return [s + fold(p if w is None else p * w) for s, w in zip(sums, weights)]


def add_counts(hot, sh_s, cnt_s):
    cnt_s[...] += lax.dot_general(hot, sh_s[...], (((1,), (1,)), ((), ())), preferred_element_type=f32)


def new_cells(genes, mom_s, cnt_s, state_ref):
    weight, s0, s1, s00, s01, s11 = [jnp.sum(mom_s[n].T, axis=0, keepdims=True) for n in range(6)]
    mu_row, mu_col, rr, rc, cc = [state_ref[n : n + 1, :] for n in range(5)]
    counts = cnt_s[0:genes, :]
    profile = (counts + pseudo_count) / (
        jnp.sum(counts, axis=0, keepdims=True) + genes * pseudo_count
    )
    denominator = weight + prior_weight
    new_row = (s0 + prior_weight * mu_row) / denominator
    new_col = (s1 + prior_weight * mu_col) / denominator
    q_rr = s00 - 2.0 * new_row * s0 + weight * new_row * new_row
    q_rc = s01 - new_row * s1 - new_col * s0 + weight * new_row * new_col
    q_cc = s11 - 2.0 * new_col * s1 + weight * new_col * new_col
    state = (
        new_row,
        new_col,
        (q_rr + prior_weight * rr) / denominator,
        (q_rc + prior_weight * rc) / denominator,
        (q_cc + prior_weight * cc) / denominator,
    )
    return profile, state, jnp.log(weight + 1.0)


def middle_kernel(
    genes,
    left_ref, mid_ref, right_ref, ltp_ref, par_ref, state_ref, told_ref,
    e_ref, m_ref, out_ref, state_out,
    hot_s, sh_s, mom_s, cnt_s, ltp_s, par_s, gl_s, sc_s, table_s, part_s,
):
    x_refs = (left_ref, mid_ref, right_ref)
    cells, tokens = sc_s.shape[1:]
    tiles = tokens // LANES
    padded = cnt_s.shape[0]
    cols = told_ref.shape[0]
    col = lax.axis_index("col")
    mom_s[...] = jnp.zeros(mom_s.shape, f32)
    cnt_s[...] = jnp.zeros(cnt_s.shape, f32)

    def posterior(source):
        for side, x_ref in enumerate(x_refs):
            hot_s[source, side] = gene_hot(x_ref, source, cells, padded)
            gl_s[side] = jnp.dot(ltp_ref[1], hot_s[source, side], preferred_element_type=f32)
        for side, x_ref in enumerate(x_refs):
            at_col = jnp.clip(col + side - 1, 0, cols - 1)
            top = row_of(told_ref, (at_col, source), 0, tiles)
            factor = row_of(told_ref, (at_col, source), tiles, tiles)
            y0, y1 = features(x_ref, source, cells, as_float(source) - 1.0, side - 1.0)
            for at in range(0, cells, 16):
                halves = []
                for a in (at, at + 8):
                    score = score_rows(a, y0, y1, gl_s.at[side], par_ref.at[1], cells)
                    count = x_ref[source, a : a + 8, :]
                    p = count * jnp.exp(jnp.minimum(score - top, 0.0)) * factor
                    sums = [mom_s[n, a : a + 8, :] for n in range(6)]
                    sums = add_moments(p, y0, y1, sums)
                    for n in range(6):
                        mom_s[n, a : a + 8, :] = sums[n]
                    halves.append(p)
                sh_s[side, at : at + 16, :] = jnp.concatenate(halves, axis=0).astype(bf16)
            add_counts(hot_s[source, side], sh_s.at[side], cnt_s)

    sources(posterior)
    profile, state, log_weight = new_cells(genes, mom_s, cnt_s, state_ref)
    state_out[...] = state_rows(state)
    table_s[...] = table_rows(profile, state, log_weight)
    load_table(table_s, ltp_s, par_s)

    def score(source):
        for side in range(3):
            gl_s[side] = jnp.dot(ltp_s[...], hot_s[source, side], preferred_element_type=f32)
        for side, x_ref in enumerate(x_refs):
            y0, y1 = features(x_ref, source, cells, as_float(source) - 1.0, side - 1.0)
            top = jnp.full((8, tokens), NEVER, f32)
            for at in range(0, cells, 8):
                value = score_rows(at, y0, y1, gl_s.at[side], par_s, cells)
                value = jnp.where(x_ref[source, at : at + 8, :] > 0.0, value, NEVER)
                sc_s[side, at : at + 8, :] = value
                top = jnp.maximum(top, value)
            top = jnp.max(top, axis=0, keepdims=True)
            total = jnp.zeros((8, tokens), f32)
            for at in range(0, cells, 8):
                e = x_ref[source, at : at + 8, :] * jnp.exp(sc_s[side, at : at + 8, :] - top)
                e_ref[source, side, at : at + 8, :] = e
                total = total + e
            total = jnp.sum(total, axis=0, keepdims=True)
            part_s[source, side] = jnp.concatenate([to_tiles(top), to_tiles(total)], axis=0)

    sources(score)
    m_ref[...] = part_s[...]
    spread_rows(part_s, out_ref)


def last_kernel(
    genes,
    left_ref, mid_ref, right_ref, e_ref, m_ref, told_ref, state_ref,
    profile_ref, cells_ref,
    sh_s, mom_s, cnt_s,
):
    x_refs = (left_ref, mid_ref, right_ref)
    cells, tokens = sh_s.shape[1:]
    tiles = tokens // LANES
    cols = told_ref.shape[0]
    col = lax.axis_index("col")
    mom_s[...] = jnp.zeros(mom_s.shape, f32)
    cnt_s[...] = jnp.zeros(cnt_s.shape, f32)
    shape = m_ref.shape[2:]
    nothing = jnp.where(lax.broadcasted_iota(i32, shape, 0) < shape[0] // 2, NEVER, 0.0)

    def posterior(source):
        for side, x_ref in enumerate(x_refs):
            parts = []
            for step in range(-1, 2):
                owner = col + side - 1 + step
                inside = (owner >= 0) & (owner < cols)
                part = told_ref[jnp.clip(owner, 0, cols - 1), source, 1 - step]
                parts.append(jnp.where(inside, part, nothing))
            top, total = joined(parts)
            scale = jnp.exp(m_ref[source, side][0:tiles] - top)
            scale = jnp.where(total > 0.0, scale / total, 0.0)
            factor = jnp.concatenate([scale[k : k + 1, :] for k in range(tiles)], axis=1)
            y0, y1 = features(x_ref, source, cells, as_float(source) - 1.0, side - 1.0)
            for at in range(0, cells, 16):
                halves = []
                for a in (at, at + 8):
                    p = e_ref[source, side, a : a + 8, :] * factor
                    sums = [mom_s[n, a : a + 8, :] for n in range(6)]
                    sums = add_moments(p, y0, y1, sums)
                    for n in range(6):
                        mom_s[n, a : a + 8, :] = sums[n]
                    halves.append(p)
                sh_s[side, at : at + 16, :] = jnp.concatenate(halves, axis=0).astype(bf16)
            add_counts(gene_hot(x_ref, source, cells, cnt_s.shape[0]), sh_s.at[side], cnt_s)

    sources(posterior)
    profile, state, log_weight = new_cells(genes, mom_s, cnt_s, state_ref)
    profile_ref[...] = jnp.log(profile)
    mu_row, mu_col, rr, rc, cc = state
    final = (mu_row, mu_col, 0.5 * jnp.log(rr), 0.5 * jnp.log(cc), rc / jnp.sqrt(rr * cc), log_weight)
    for n, row in enumerate(final):
        cells_ref[n] = row


def body(
    positions, genes, candidates, block_counts, profile_weights, centroids, spreads, correlation
):
    gene_total = profile_weights.shape[0]
    cells = profile_weights.shape[3]
    tokens, slots = candidates.shape[2:]
    tiles = tokens // LANES
    rows = lax.axis_size("row")
    padded = padded_to(gene_total, LANES)
    pairs = 9 * tokens * cells
    table = ((padded_to(gene_total, 8) + 8, cells), f32)
    state = ((8, cells), f32)
    vmem = pltpu.VMEM

    packed, table_own, state_own = call(
        pack_kernel, "pack", [((slots + FEATURES, tokens), f32), table, state],
        [ANY] * 8,
        [
            vmem((1, block_counts.shape[2]), i32),
            vmem((tokens, slots), i32),
            vmem((2 * tiles, LANES), f32),
            vmem((tiles, LANES), i32),
            vmem((gene_total, cells), f32),
            vmem((2, cells), f32),
            vmem((2, cells), f32),
            vmem((1, cells), f32),
            pltpu.SemaphoreType.DMA((8,)),
        ],
        tokens * slots,
        [
            pltpu.with_memory_space_constraint(a, pltpu.HBM)
            for a in (
                block_counts.reshape(1, -1),
                candidates.reshape(tokens, slots),
                positions.reshape(2 * tiles, LANES),
                genes.reshape(tiles, LANES),
                profile_weights.reshape(gene_total, cells),
                centroids.reshape(2, cells),
                spreads.reshape(2, cells),
                correlation.reshape(1, cells),
            )
        ],
    )
    from_up = shifted(packed, "row", 1)
    from_down = shifted(packed, "row", -1)
    table_left = shifted(table_own, "col", 1)
    table_right = shifted(table_own, "col", -1)
    ltp, par = call(
        tables_kernel, "tables",
        [((3, PARTS * cells, padded), bf16), ((3, 6, cells, LANES), f32)], [VMEM] * 3, [],
        tokens * slots, (table_left, table_own, table_right),
    )
    one = ((cells + FEATURES, tokens), f32)
    three = ((3, cells + FEATURES, tokens), f32)
    count_scratch = [vmem((tiles, slots + 8, LANES), i32)] * 2
    own = call(
        functools.partial(own_counts_kernel, cells), "own_counts", [one] * 3, [VMEM],
        count_scratch, pairs * 40, (packed,),
    )
    to_left, mid, to_right = call(
        functools.partial(counts_kernel, cells), "counts", [three] * 3, [VMEM] * 5 + [ANY],
        count_scratch, pairs * 80, (from_up, from_down, *own, ltp),
    )
    from_right = shifted(to_left, "col", -1)
    from_left = shifted(to_right, "col", 1)

    chunk = (2 * tiles, LANES)
    parts, = call(
        row_parts_kernel, "row_parts", [((rows, 3) + chunk, f32)], [VMEM] * 5,
        [
            vmem((3,) + chunk, f32),
            vmem((3, PARTS * cells, tokens), f32),
            vmem((3, cells, tokens), f32),
        ],
        pairs * 100,
        (to_left, mid, to_right, ltp, par),
    )
    back = lax.all_to_all(parts, "row", 0, 0)
    sums, = call(row_join_kernel, "row_join", [((3,) + chunk, f32)], [VMEM], [], tokens * 100, (back,))
    told_all = lax.all_gather(sums, "col", axis=0)

    x = (from_left, mid, from_right)
    sum_scratch = [
        vmem((3, cells, tokens), bf16),
        vmem((6, cells, LANES), f32),
        vmem((padded, cells), f32),
    ]
    e, m, parts, state_own = call(
        functools.partial(middle_kernel, gene_total), "middle",
        [((3, 3, cells, tokens), f32), ((3, 3) + chunk, f32), ((rows, 3, 3) + chunk, f32), state],
        [VMEM] * 7,
        [vmem((3, 3, padded, tokens), bf16)] + sum_scratch + [
            vmem((PARTS * cells, padded), bf16),
            vmem((6, cells, LANES), f32),
            vmem((3, PARTS * cells, tokens), f32),
            vmem((3, cells, tokens), f32),
            vmem(*table),
            vmem((3, 3) + chunk, f32),
        ],
        pairs * 200,
        (*x, ltp, par, state_own, told_all),
    )
    back = lax.all_to_all(parts, "row", 0, 0)
    sums, = call(part_join_kernel, "part_join", [((3, 3) + chunk, f32)], [VMEM], [], tokens * 100, (back,))
    told_all = lax.all_gather(sums, "col", axis=0)
    final_profile, final_cells = call(
        functools.partial(last_kernel, gene_total), "last",
        [((gene_total, cells), f32), ((6, 1, cells), f32)],
        [VMEM] * 7, sum_scratch, pairs * 100,
        (*x, e, m, told_all, state_own),
    )
    return (final_profile.reshape(gene_total, 1, 1, cells), final_cells.reshape(6, 1, 1, cells))


def solution(mesh):
    tiles = P(("groups", "row"), "col")
    stacked = P(None, ("groups", "row"), "col", None)
    return jax.shard_map(
        body,
        mesh=mesh,
        in_specs=(
            stacked,
            P(("groups", "row"), "col", None),
            P(("groups", "row"), "col", None, None),
            P(("groups", "row"), "col", None),
            stacked,
            stacked,
            stacked,
            P(("groups", "row"), "col", None),
        ),
        out_specs=(stacked, stacked),
        check_vma=False,
    )
```

```python
import functools

import jax
import jax.numpy as jnp
from jax import lax
from jax.experimental import pallas as pl
from jax.experimental.pallas import tpu as pltpu
from jax.sharding import PartitionSpec as P

BLOCK = 256
LANES = 128
FEATURES = 8
PARTS = 2
NEVER = -1e30

pseudo_count = 0.05
prior_weight = 1.0

f32 = jnp.float32
bf16 = jnp.bfloat16
i32 = jnp.int32


def swapped(to_first, to_second, axis):
    count = lax.axis_size(axis)
    out = []
    for start, x in enumerate((to_first, to_second)):
        pairs = [p for i in range(start, count - 1, 2) for p in ((i, i + 1), (i + 1, i))]
        out.append(lax.ppermute(x, axis, pairs))
    return out


def params(mib=40):
    return pltpu.CompilerParams(vmem_limit_bytes=mib << 20)


def cost(flops, size):
    return pl.CostEstimate(flops=flops, bytes_accessed=size, transcendentals=0)


def call(kernel, name, outs, in_specs, scratch, flops, args):
    shapes = [jax.ShapeDtypeStruct(s, d) for s, d in outs]
    return pl.pallas_call(
        kernel,
        name=name,
        out_shape=shapes,
        in_specs=in_specs,
        out_specs=[pl.BlockSpec(memory_space=pltpu.VMEM)] * len(shapes),
        scratch_shapes=scratch,
        compiler_params=params(),
        cost_estimate=cost(flops, 1 << 20),
    )(*args)


VMEM = pl.BlockSpec(memory_space=pltpu.VMEM)
SMEM = pl.BlockSpec(memory_space=pltpu.SMEM)
ANY = pl.BlockSpec(memory_space=pltpu.HBM)


def lane_tile(k):
    return pl.ds(k * LANES, LANES)


def padded_to(size, unit):
    return -(-size // unit) * unit


def order(axis):
    first = 2 * (1 - lax.rem(lax.axis_index(axis), 2))
    return (first, 1, 2 - first)


def as_float(x):
    return x.astype(f32) if hasattr(x, "astype") else float(x)


def table_rows(profile, state, log_weight):
    genes, cells = profile.shape
    mu_row, mu_col, rr, rc, cc = state
    det = rr * cc - rc * rc
    rows = [jnp.log(profile)]
    if genes % 8:
        rows.append(jnp.zeros((-genes % 8, cells), f32))
    rows += [
        mu_row,
        mu_col,
        -0.5 * (cc / det),
        rc / det,
        -0.5 * (rr / det),
        log_weight - 0.5 * jnp.log(det),
        jnp.zeros((2, cells), f32),
    ]
    return jnp.concatenate(rows, axis=0)


def state_rows(state):
    return jnp.concatenate(list(state) + [jnp.zeros((3, state[0].shape[1]), f32)], axis=0)


def pack_kernel(
    count_hbm, cand_hbm, pos_hbm, gene_hbm, weight_hbm, centre_hbm, spread_hbm, corr_hbm,
    out_ref, table_ref, state_ref,
    count_ref, cand_ref, pos_ref, gene_ref, weight_ref, centre_ref, spread_ref, corr_ref, sems,
):
    pairs = (
        (count_hbm, count_ref), (cand_hbm, cand_ref), (pos_hbm, pos_ref), (gene_hbm, gene_ref), (weight_hbm, weight_ref),
        (centre_hbm, centre_ref), (spread_hbm, spread_ref), (corr_hbm, corr_ref),
    )
    copies = [pltpu.make_async_copy(a, b, sems.at[n]) for n, (a, b) in enumerate(pairs)]
    for copy in copies:
        copy.start()
    for copy in copies[:4]:
        copy.wait()
    tokens, slots = cand_ref.shape
    tiles = tokens // LANES
    out_ref[0:slots, :] = cand_ref[...].astype(f32).T
    lane = lax.broadcasted_iota(i32, (1, LANES), 1)
    for k in range(tiles):
        start = k * LANES
        live = (start % BLOCK + lane) < count_ref[:, start // BLOCK : start // BLOCK + 1]
        rows = [
            pos_ref[k : k + 1, :],
            pos_ref[tiles + k : tiles + k + 1, :],
            gene_ref[k : k + 1, :].astype(f32),
            live.astype(f32),
            jnp.zeros((FEATURES - 4, LANES), f32),
        ]
        out_ref[slots : slots + FEATURES, lane_tile(k)] = jnp.concatenate(rows, axis=0)
    for copy in copies[4:]:
        copy.wait()
    weights = weight_ref[...]
    spread_row, spread_col = spread_ref[0:1, :], spread_ref[1:2, :]
    state = (
        centre_ref[0:1, :],
        centre_ref[1:2, :],
        spread_row * spread_row,
        corr_ref[0:1, :] * spread_row * spread_col,
        spread_col * spread_col,
    )
    state_ref[...] = state_rows(state)
    profile = weights / jnp.sum(weights, axis=0, keepdims=True)
    table_ref[...] = table_rows(profile, state, jnp.zeros_like(spread_row))


def count_source(source, z_ref, cells, outs, word_s, unit_s):
    rows, tokens = z_ref.shape
    slots = rows - FEATURES
    words = cells // 8
    shift = cells.bit_length() - 1
    word_shift = words.bit_length() - 1
    held = 3 * words // 8
    per_tile = words // 8
    sub = lax.broadcasted_iota(i32, (8, LANES), 0)
    nibbles = jnp.full((8, LANES), 0x0F0F0F0F, i32)
    first = order("col")[0]
    for k in range(tokens // LANES):
        local = z_ref[0:slots, lane_tile(k)].astype(i32) - (2 - source) * 3 * cells
        place = first + (local >> shift) * (1 - first)
        word_s[k, 0:slots, :] = place * words + (local & (words - 1))
        unit_s[k, 0:slots, :] = 1 << (((local & (cells - 1)) >> word_shift) * 4)

    def some(k, start, amount, carry):
        low, high = carry
        word = [jnp.zeros((8, LANES), i32) for _ in range(held)]
        for j in range(amount):
            which = word_s[k, pl.ds(start + j, 8, stride=0), :]
            unit = unit_s[k, pl.ds(start + j, 8, stride=0), :]
            for n in range(held):
                word[n] = word[n] + jnp.where(which == sub + 8 * n, unit, 0)
        low = [a + (w & nibbles) for a, w in zip(low, word)]
        high = [a + ((w >> 4) & nibbles) for a, w in zip(high, word)]
        return low, high

    for k in range(tokens // LANES):
        zero = [jnp.zeros((8, LANES), i32) for _ in range(held)]
        whole = slots // 15
        carry = lax.fori_loop(
            0, whole, lambda g, carry: some(k, g * 15, 15, carry), (zero, list(zero))
        )
        if slots % 15:
            carry = some(k, whole * 15, slots % 15, carry)
        low, high = carry
        live = z_ref[slots + 3 : slots + 4, lane_tile(k)]
        for n in range(held):
            for field in range(8):
                part = low[n] if field % 2 == 0 else high[n]
                value = ((part >> (8 * (field // 2))) & 255).astype(f32) * live
                row = field * words + (n % per_tile) * 8
                outs[n // per_tile][row : row + 8, lane_tile(k)] = value
    for out in outs:
        out[cells : cells + FEATURES, :] = z_ref[slots : slots + FEATURES, :]


def own_counts_kernel(cells, own_ref, first_ref, mid_ref, second_ref, word_s, unit_s):
    count_source(1, own_ref, cells, (first_ref, mid_ref, second_ref), word_s, unit_s)


def counts_kernel(
    cells, first_ref, second_ref, own_first, own_mid, own_second, ltp_hbm,
    to_first, mid_ref, to_second, word_s, unit_s,
):
    outs = (to_first, mid_ref, to_second)
    for out, own in zip(outs, (own_first, own_mid, own_second)):
        out[1] = own[...]
    first, _, second = order("row")
    for q, source, z_ref in ((0, first, first_ref), (2, second, second_ref)):
        count_source(source, z_ref, cells, [out.at[q] for out in outs], word_s, unit_s)


def load_table(table_ref, ltp_s, par_s):
    cells = table_ref.shape[1]
    padded = ltp_s.shape[1]
    genes = table_ref.shape[0] - 8
    logs = [table_ref[0:genes, :]]
    if padded > genes:
        logs.append(jnp.zeros((padded - genes, cells), f32))
    rest = jnp.concatenate(logs, axis=0).T
    for part in range(PARTS):
        piece = rest.astype(bf16)
        ltp_s[part * cells : (part + 1) * cells, :] = piece
        if part + 1 < PARTS:
            rest = rest - piece.astype(f32)
    rows = [table_ref[genes : genes + 8, :], jnp.zeros((LANES - 8, cells), f32)]
    columns = jnp.concatenate(rows, axis=0).T
    for n in range(6):
        par_s[n] = jnp.broadcast_to(columns[:, n : n + 1], (cells, LANES))


def tables_kernel(first_ref, own_ref, second_ref, ltp_ref, par_ref):
    for side, table in enumerate((first_ref, own_ref, second_ref)):
        load_table(table, ltp_ref.at[side], par_ref.at[side])


def gene_hot(x_ref, source, cells, padded):
    tokens = x_ref.shape[2]
    gene = x_ref[source, cells + 2 : cells + 3, :].astype(i32).astype(jnp.int16)
    axis = lax.broadcasted_iota(jnp.int16, (padded, tokens), 0)
    return jnp.where(axis == gene, jnp.ones((), bf16), jnp.zeros((), bf16))


def features(x_ref, source, cells, row_step, col_step):
    y0 = x_ref[source, cells : cells + 1, :] + row_step
    y1 = x_ref[source, cells + 1 : cells + 2, :] + col_step
    return y0, y1


def score_rows(at, y0, y1, gl_s, par_s, cells):
    tiles = y0.shape[1] // LANES
    p = [jnp.concatenate([par_s[n, at : at + 8, :]] * tiles, axis=1) for n in range(6)]
    d0 = y0 - p[0]
    d1 = y1 - p[1]
    logs = gl_s[at : at + 8, :]
    for part in range(1, PARTS):
        logs = logs + gl_s[part * cells + at : part * cells + at + 8, :]
    return logs + p[5] + (d0 * (p[2] * d0 + p[3] * d1) + p[4] * d1 * d1)


def row_of(ref, index, first, tiles):
    return jnp.concatenate([ref[index + (pl.ds(first + k, 1), slice(None))] for k in range(tiles)], axis=1)


def to_tiles(row):
    return jnp.concatenate([row[:, k * LANES : (k + 1) * LANES] for k in range(row.shape[1] // LANES)], axis=0)


def spread_rows(part_s, out_ref):
    rows = out_ref.shape[0]
    half = part_s.shape[-2] // 2
    shape = out_ref.shape[2:]
    level = lax.broadcasted_iota(i32, shape, len(shape) - 2)
    nothing = jnp.where(level < half, NEVER, 0.0)
    row = lax.axis_index("row")

    @pl.loop(0, rows)
    def _(at):
        for slot in range(3):
            source = at - row + slot
            inside = (source >= 0) & (source < 3)
            out_ref[at, slot] = jnp.where(inside, part_s[jnp.clip(source, 0, 2)], nothing)


def joined(parts):
    half = parts[0].shape[-2] // 2
    tops = [p[..., 0:half, :] for p in parts]
    top = functools.reduce(jnp.maximum, tops)
    total = sum(p[..., half:, :] * jnp.exp(m - top) for p, m in zip(parts, tops))
    return top, total


def gather_rows(in_ref):
    rows = in_ref.shape[0]
    row = lax.axis_index("row")
    shape = in_ref.shape[1:]
    half = shape[-2] // 2
    level = lax.broadcasted_iota(i32, shape, len(shape) - 2)
    nothing = jnp.where(level < half, NEVER, 0.0)
    parts = []
    for step in range(-2, 3):
        inside = (row + step >= 0) & (row + step < rows)
        parts.append(jnp.where(inside, in_ref[jnp.clip(row + step, 0, rows - 1)], nothing))
    return joined(parts)


def told(top, total):
    return jnp.concatenate([top, jnp.where(total > 0.0, 1.0 / total, 0.0)], axis=-2)


def row_parts_kernel(
    first_ref, mid_ref, second_ref, ltp_s, par_s, out_ref, part_s, gl_s, sc_s
):
    x_refs = (first_ref, mid_ref, second_ref)
    cells, tokens = sc_s.shape[1:]

    for q, source in enumerate(order("row")):
        hot = gene_hot(mid_ref, q, cells, ltp_s.shape[2])
        for side in range(3):
            gl_s[side] = jnp.dot(ltp_s[side], hot, preferred_element_type=f32)
        top = jnp.full((8, tokens), NEVER, f32)
        for side, at_side in enumerate(order("col")):
            y0, y1 = features(mid_ref, q, cells, as_float(source) - 1.0, 1.0 - as_float(at_side))
            for at in range(0, cells, 8):
                score = score_rows(at, y0, y1, gl_s.at[side], par_s.at[side], cells)
                score = jnp.where(x_refs[side][q, at : at + 8, :] > 0.0, score, NEVER)
                sc_s[side, at : at + 8, :] = score
                top = jnp.maximum(top, score)
        top = jnp.max(top, axis=0, keepdims=True)
        total = jnp.zeros((8, tokens), f32)
        for side in range(3):
            for at in range(0, cells, 8):
                count = x_refs[side][q, at : at + 8, :]
                total = total + count * jnp.exp(sc_s[side, at : at + 8, :] - top)
        total = jnp.sum(total, axis=0, keepdims=True)
        part_s[source] = jnp.concatenate([to_tiles(top), to_tiles(total)], axis=0)
    spread_rows(part_s, out_ref)


def row_join_kernel(in_ref, out_ref):
    out_ref[...] = told(*gather_rows(in_ref))


def part_join_kernel(in_ref, out_ref):
    out_ref[...] = jnp.concatenate(gather_rows(in_ref), axis=-2)


def add_moments(p, y0, y1, sums):
    def fold(x):
        parts = [x[:, k * LANES : (k + 1) * LANES] for k in range(x.shape[1] // LANES)]
        return functools.reduce(jnp.add, parts)

    weights = (None, y0, y1, y0 * y0, y0 * y1, y1 * y1)
    return [s + fold(p if w is None else p * w) for s, w in zip(sums, weights)]


def add_counts(hot, sh_s, cnt_s):
    cnt_s[...] += lax.dot_general(hot, sh_s[...], (((1,), (1,)), ((), ())), preferred_element_type=f32)


def new_cells(genes, mom_s, cnt_s, state_ref):
    weight, s0, s1, s00, s01, s11 = [jnp.sum(mom_s[n].T, axis=0, keepdims=True) for n in range(6)]
    mu_row, mu_col, rr, rc, cc = [state_ref[n : n + 1, :] for n in range(5)]
    counts = cnt_s[0:genes, :]
    profile = (counts + pseudo_count) / (
        jnp.sum(counts, axis=0, keepdims=True) + genes * pseudo_count
    )
    denominator = weight + prior_weight
    new_row = (s0 + prior_weight * mu_row) / denominator
    new_col = (s1 + prior_weight * mu_col) / denominator
    q_rr = s00 - 2.0 * new_row * s0 + weight * new_row * new_row
    q_rc = s01 - new_row * s1 - new_col * s0 + weight * new_row * new_col
    q_cc = s11 - 2.0 * new_col * s1 + weight * new_col * new_col
    state = (
        new_row,
        new_col,
        (q_rr + prior_weight * rr) / denominator,
        (q_rc + prior_weight * rc) / denominator,
        (q_cc + prior_weight * cc) / denominator,
    )
    return profile, state, jnp.log(weight + 1.0)


def middle_kernel(
    genes,
    first_ref, mid_ref, second_ref, ltp_ref, par_ref, state_ref, told_ref,
    e_ref, m_ref, out_ref, state_out,
    hot_s, sh_s, mom_s, cnt_s, ltp_s, par_s, gl_s, sc_s, table_s, part_s,
):
    x_refs = (first_ref, mid_ref, second_ref)
    cells, tokens = sc_s.shape[1:]
    tiles = tokens // LANES
    padded = cnt_s.shape[0]
    cols = told_ref.shape[0]
    col = lax.axis_index("col")
    mom_s[...] = jnp.zeros(mom_s.shape, f32)
    cnt_s[...] = jnp.zeros(cnt_s.shape, f32)

    for q, source in enumerate(order("row")):
        for side, x_ref in enumerate(x_refs):
            hot_s[q, side] = gene_hot(x_ref, q, cells, padded)
            gl_s[side] = jnp.dot(ltp_ref[1], hot_s[q, side], preferred_element_type=f32)
        for side, (at_side, x_ref) in enumerate(zip(order("col"), x_refs)):
            at_col = jnp.clip(col + at_side - 1, 0, cols - 1)
            top = row_of(told_ref, (at_col, source), 0, tiles)
            factor = row_of(told_ref, (at_col, source), tiles, tiles)
            y0, y1 = features(x_ref, q, cells, as_float(source) - 1.0, as_float(at_side) - 1.0)
            for at in range(0, cells, 16):
                halves = []
                for a in (at, at + 8):
                    score = score_rows(a, y0, y1, gl_s.at[side], par_ref.at[1], cells)
                    count = x_ref[q, a : a + 8, :]
                    p = count * jnp.exp(jnp.minimum(score - top, 0.0)) * factor
                    sums = [mom_s[n, a : a + 8, :] for n in range(6)]
                    sums = add_moments(p, y0, y1, sums)
                    for n in range(6):
                        mom_s[n, a : a + 8, :] = sums[n]
                    halves.append(p)
                sh_s[side, at : at + 16, :] = jnp.concatenate(halves, axis=0).astype(bf16)
            add_counts(hot_s[q, side], sh_s.at[side], cnt_s)

    profile, state, log_weight = new_cells(genes, mom_s, cnt_s, state_ref)
    state_out[...] = state_rows(state)
    table_s[...] = table_rows(profile, state, log_weight)
    load_table(table_s, ltp_s, par_s)

    for q, source in enumerate(order("row")):
        for side in range(3):
            gl_s[side] = jnp.dot(ltp_s[...], hot_s[q, side], preferred_element_type=f32)
        for side, (at_side, x_ref) in enumerate(zip(order("col"), x_refs)):
            y0, y1 = features(x_ref, q, cells, as_float(source) - 1.0, as_float(at_side) - 1.0)
            top = jnp.full((8, tokens), NEVER, f32)
            for at in range(0, cells, 8):
                value = score_rows(at, y0, y1, gl_s.at[side], par_s, cells)
                value = jnp.where(x_ref[q, at : at + 8, :] > 0.0, value, NEVER)
                sc_s[side, at : at + 8, :] = value
                top = jnp.maximum(top, value)
            top = jnp.max(top, axis=0, keepdims=True)
            total = jnp.zeros((8, tokens), f32)
            for at in range(0, cells, 8):
                e = x_ref[q, at : at + 8, :] * jnp.exp(sc_s[side, at : at + 8, :] - top)
                e_ref[q, side, at : at + 8, :] = e
                total = total + e
            total = jnp.sum(total, axis=0, keepdims=True)
            part_s[source, at_side] = jnp.concatenate([to_tiles(top), to_tiles(total)], axis=0)

    m_ref[...] = part_s[...]
    spread_rows(part_s, out_ref)


def last_kernel(
    genes,
    first_ref, mid_ref, second_ref, e_ref, m_ref, told_ref, state_ref,
    profile_ref, cells_ref,
    sh_s, mom_s, cnt_s,
):
    x_refs = (first_ref, mid_ref, second_ref)
    cells, tokens = sh_s.shape[1:]
    tiles = tokens // LANES
    cols = told_ref.shape[0]
    col = lax.axis_index("col")
    mom_s[...] = jnp.zeros(mom_s.shape, f32)
    cnt_s[...] = jnp.zeros(cnt_s.shape, f32)
    shape = m_ref.shape[2:]
    nothing = jnp.where(lax.broadcasted_iota(i32, shape, 0) < shape[0] // 2, NEVER, 0.0)

    for q, source in enumerate(order("row")):
        for side, (at_side, x_ref) in enumerate(zip(order("col"), x_refs)):
            parts = []
            for step in range(-1, 2):
                owner = col + at_side - 1 + step
                inside = (owner >= 0) & (owner < cols)
                part = told_ref[jnp.clip(owner, 0, cols - 1), source, 1 - step]
                parts.append(jnp.where(inside, part, nothing))
            top, total = joined(parts)
            scale = jnp.exp(m_ref[source, at_side][0:tiles] - top)
            scale = jnp.where(total > 0.0, scale / total, 0.0)
            factor = jnp.concatenate([scale[k : k + 1, :] for k in range(tiles)], axis=1)
            y0, y1 = features(x_ref, q, cells, as_float(source) - 1.0, as_float(at_side) - 1.0)
            for at in range(0, cells, 16):
                halves = []
                for a in (at, at + 8):
                    p = e_ref[q, side, a : a + 8, :] * factor
                    sums = [mom_s[n, a : a + 8, :] for n in range(6)]
                    sums = add_moments(p, y0, y1, sums)
                    for n in range(6):
                        mom_s[n, a : a + 8, :] = sums[n]
                    halves.append(p)
                sh_s[side, at : at + 16, :] = jnp.concatenate(halves, axis=0).astype(bf16)
            add_counts(gene_hot(x_ref, q, cells, cnt_s.shape[0]), sh_s.at[side], cnt_s)

    profile, state, log_weight = new_cells(genes, mom_s, cnt_s, state_ref)
    profile_ref[...] = jnp.log(profile)
    mu_row, mu_col, rr, rc, cc = state
    final = (mu_row, mu_col, 0.5 * jnp.log(rr), 0.5 * jnp.log(cc), rc / jnp.sqrt(rr * cc), log_weight)
    for n, row in enumerate(final):
        cells_ref[n] = row


def body(
    positions, genes, candidates, block_counts, profile_weights, centroids, spreads, correlation
):
    gene_total = profile_weights.shape[0]
    cells = profile_weights.shape[3]
    tokens, slots = candidates.shape[2:]
    tiles = tokens // LANES
    rows = lax.axis_size("row")
    padded = padded_to(gene_total, LANES)
    pairs = 9 * tokens * cells
    table = ((padded_to(gene_total, 8) + 8, cells), f32)
    state = ((8, cells), f32)
    vmem = pltpu.VMEM

    packed, table_own, state_own = call(
        pack_kernel, "pack", [((slots + FEATURES, tokens), f32), table, state],
        [ANY] * 8,
        [
            vmem((1, block_counts.shape[2]), i32),
            vmem((tokens, slots), i32),
            vmem((2 * tiles, LANES), f32),
            vmem((tiles, LANES), i32),
            vmem((gene_total, cells), f32),
            vmem((2, cells), f32),
            vmem((2, cells), f32),
            vmem((1, cells), f32),
            pltpu.SemaphoreType.DMA((8,)),
        ],
        tokens * slots,
        [
            pltpu.with_memory_space_constraint(a, pltpu.HBM)
            for a in (
                block_counts.reshape(1, -1),
                candidates.reshape(tokens, slots),
                positions.reshape(2 * tiles, LANES),
                genes.reshape(tiles, LANES),
                profile_weights.reshape(gene_total, cells),
                centroids.reshape(2, cells),
                spreads.reshape(2, cells),
                correlation.reshape(1, cells),
            )
        ],
    )
    row_first, row_second = swapped(packed, packed, "row")
    table_first, table_second = swapped(table_own, table_own, "col")
    ltp, par = call(
        tables_kernel, "tables",
        [((3, PARTS * cells, padded), bf16), ((3, 6, cells, LANES), f32)], [VMEM] * 3, [],
        tokens * slots, (table_first, table_own, table_second),
    )
    one = ((cells + FEATURES, tokens), f32)
    three = ((3, cells + FEATURES, tokens), f32)
    count_scratch = [vmem((tiles, slots + 8, LANES), i32)] * 2
    own = call(
        functools.partial(own_counts_kernel, cells), "own_counts", [one] * 3, [VMEM],
        count_scratch, pairs * 40, (packed,),
    )
    to_first, mid, to_second = call(
        functools.partial(counts_kernel, cells), "counts", [three] * 3, [VMEM] * 5 + [ANY],
        count_scratch, pairs * 80, (row_first, row_second, *own, ltp),
    )
    from_first, from_second = swapped(to_first, to_second, "col")

    chunk = (2 * tiles, LANES)
    parts, = call(
        row_parts_kernel, "row_parts", [((rows, 3) + chunk, f32)], [VMEM] * 5,
        [
            vmem((3,) + chunk, f32),
            vmem((3, PARTS * cells, tokens), f32),
            vmem((3, cells, tokens), f32),
        ],
        pairs * 100,
        (to_first, mid, to_second, ltp, par),
    )
    back = lax.all_to_all(parts, "row", 0, 0)
    sums, = call(row_join_kernel, "row_join", [((3,) + chunk, f32)], [VMEM], [], tokens * 100, (back,))
    told_all = lax.all_gather(sums, "col", axis=0)

    x = (from_first, mid, from_second)
    sum_scratch = [
        vmem((3, cells, tokens), bf16),
        vmem((6, cells, LANES), f32),
        vmem((padded, cells), f32),
    ]
    e, m, parts, state_own = call(
        functools.partial(middle_kernel, gene_total), "middle",
        [((3, 3, cells, tokens), f32), ((3, 3) + chunk, f32), ((rows, 3, 3) + chunk, f32), state],
        [VMEM] * 7,
        [vmem((3, 3, padded, tokens), bf16)] + sum_scratch + [
            vmem((PARTS * cells, padded), bf16),
            vmem((6, cells, LANES), f32),
            vmem((3, PARTS * cells, tokens), f32),
            vmem((3, cells, tokens), f32),
            vmem(*table),
            vmem((3, 3) + chunk, f32),
        ],
        pairs * 200,
        (*x, ltp, par, state_own, told_all),
    )
    back = lax.all_to_all(parts, "row", 0, 0)
    sums, = call(part_join_kernel, "part_join", [((3, 3) + chunk, f32)], [VMEM], [], tokens * 100, (back,))
    told_all = lax.all_gather(sums, "col", axis=0)
    final_profile, final_cells = call(
        functools.partial(last_kernel, gene_total), "last",
        [((gene_total, cells), f32), ((6, 1, cells), f32)],
        [VMEM] * 7, sum_scratch, pairs * 100,
        (*x, e, m, told_all, state_own),
    )
    return (final_profile.reshape(gene_total, 1, 1, cells), final_cells.reshape(6, 1, 1, cells))


def solution(mesh):
    tiles = P(("groups", "row"), "col")
    stacked = P(None, ("groups", "row"), "col", None)
    return jax.shard_map(
        body,
        mesh=mesh,
        in_specs=(
            stacked,
            P(("groups", "row"), "col", None),
            P(("groups", "row"), "col", None, None),
            P(("groups", "row"), "col", None),
            stacked,
            stacked,
            stacked,
            P(("groups", "row"), "col", None),
        ),
        out_specs=(stacked, stacked),
        check_vma=False,
    )
```

```python
import functools

import jax
import jax.numpy as jnp
from jax import lax
from jax.experimental import pallas as pl
from jax.experimental.pallas import tpu as pltpu
from jax.sharding import PartitionSpec as P

BLOCK = 256
LANES = 128
FEATURES = 8
PARTS = 2
NEVER = -1e30

pseudo_count = 0.05
prior_weight = 1.0

f32 = jnp.float32
bf16 = jnp.bfloat16
i32 = jnp.int32


def swapped(to_first, to_second, axis):
    count = lax.axis_size(axis)
    out = []
    for start, x in enumerate((to_first, to_second)):
        pairs = [p for i in range(start, count - 1, 2) for p in ((i, i + 1), (i + 1, i))]
        out.append(lax.ppermute(x, axis, pairs))
    return out


def params(mib=40):
    return pltpu.CompilerParams(vmem_limit_bytes=mib << 20)


def cost(flops, size):
    return pl.CostEstimate(flops=flops, bytes_accessed=size, transcendentals=0)


def call(kernel, name, outs, in_specs, scratch, flops, args):
    shapes = [jax.ShapeDtypeStruct(s, d) for s, d in outs]
    return pl.pallas_call(
        kernel,
        name=name,
        out_shape=shapes,
        in_specs=in_specs,
        out_specs=[pl.BlockSpec(memory_space=pltpu.VMEM)] * len(shapes),
        scratch_shapes=scratch,
        compiler_params=params(),
        cost_estimate=cost(flops, 1 << 20),
    )(*args)


VMEM = pl.BlockSpec(memory_space=pltpu.VMEM)
SMEM = pl.BlockSpec(memory_space=pltpu.SMEM)
ANY = pl.BlockSpec(memory_space=pltpu.HBM)


def lane_tile(k):
    return pl.ds(k * LANES, LANES)


def padded_to(size, unit):
    return -(-size // unit) * unit


def order(axis):
    first = 2 * (1 - lax.rem(lax.axis_index(axis), 2))
    return (first, 1, 2 - first)


def as_float(x):
    return x.astype(f32) if hasattr(x, "astype") else float(x)


def table_rows(profile, state, log_weight):
    genes, cells = profile.shape
    mu_row, mu_col, rr, rc, cc = state
    det = rr * cc - rc * rc
    rows = [jnp.log(profile)]
    if genes % 8:
        rows.append(jnp.zeros((-genes % 8, cells), f32))
    rows += [
        mu_row,
        mu_col,
        -0.5 * (cc / det),
        rc / det,
        -0.5 * (rr / det),
        log_weight - 0.5 * jnp.log(det),
        jnp.zeros((2, cells), f32),
    ]
    return jnp.concatenate(rows, axis=0)


def state_rows(state):
    return jnp.concatenate(list(state) + [jnp.zeros((3, state[0].shape[1]), f32)], axis=0)


def pack_kernel(
    count_hbm, cand_hbm, pos_hbm, gene_hbm, weight_hbm, centre_hbm, spread_hbm, corr_hbm,
    out_ref, table_ref, state_ref,
    count_ref, cand_ref, pos_ref, gene_ref, weight_ref, centre_ref, spread_ref, corr_ref, sems,
):
    pairs = (
        (count_hbm, count_ref), (cand_hbm, cand_ref), (pos_hbm, pos_ref), (gene_hbm, gene_ref), (weight_hbm, weight_ref),
        (centre_hbm, centre_ref), (spread_hbm, spread_ref), (corr_hbm, corr_ref),
    )
    copies = [pltpu.make_async_copy(a, b, sems.at[n]) for n, (a, b) in enumerate(pairs)]
    for copy in copies:
        copy.start()
    for copy in copies[:4]:
        copy.wait()
    tokens, slots = cand_ref.shape
    tiles = tokens // LANES
    out_ref[0:slots, :] = cand_ref[...].astype(f32).T
    lane = lax.broadcasted_iota(i32, (1, LANES), 1)
    for k in range(tiles):
        start = k * LANES
        live = (start % BLOCK + lane) < count_ref[:, start // BLOCK : start // BLOCK + 1]
        rows = [
            pos_ref[k : k + 1, :],
            pos_ref[tiles + k : tiles + k + 1, :],
            gene_ref[k : k + 1, :].astype(f32),
            live.astype(f32),
            jnp.zeros((FEATURES - 4, LANES), f32),
        ]
        out_ref[slots : slots + FEATURES, lane_tile(k)] = jnp.concatenate(rows, axis=0)
    for copy in copies[4:]:
        copy.wait()
    weights = weight_ref[...]
    spread_row, spread_col = spread_ref[0:1, :], spread_ref[1:2, :]
    state = (
        centre_ref[0:1, :],
        centre_ref[1:2, :],
        spread_row * spread_row,
        corr_ref[0:1, :] * spread_row * spread_col,
        spread_col * spread_col,
    )
    state_ref[...] = state_rows(state)
    profile = weights / jnp.sum(weights, axis=0, keepdims=True)
    table_ref[...] = table_rows(profile, state, jnp.zeros_like(spread_row))


def count_source(source, z_ref, cells, outs, word_s, unit_s):
    rows, tokens = z_ref.shape
    slots = rows - FEATURES
    words = cells // 8
    shift = cells.bit_length() - 1
    word_shift = words.bit_length() - 1
    held = 3 * words // 8
    per_tile = words // 8
    sub = lax.broadcasted_iota(i32, (8, LANES), 0)
    nibbles = jnp.full((8, LANES), 0x0F0F0F0F, i32)
    first = order("col")[0]
    for k in range(tokens // LANES):
        local = z_ref[0:slots, lane_tile(k)].astype(i32) - (2 - source) * 3 * cells
        place = first + (local >> shift) * (1 - first)
        word_s[k, 0:slots, :] = place * words + (local & (words - 1))
        unit_s[k, 0:slots, :] = 1 << (((local & (cells - 1)) >> word_shift) * 4)

    def some(k, start, amount, carry):
        low, high = carry
        word = [jnp.zeros((8, LANES), i32) for _ in range(held)]
        for j in range(amount):
            which = word_s[k, pl.ds(start + j, 8, stride=0), :]
            unit = unit_s[k, pl.ds(start + j, 8, stride=0), :]
            for n in range(held):
                word[n] = word[n] + jnp.where(which == sub + 8 * n, unit, 0)
        low = [a + (w & nibbles) for a, w in zip(low, word)]
        high = [a + ((w >> 4) & nibbles) for a, w in zip(high, word)]
        return low, high

    for k in range(tokens // LANES):
        zero = [jnp.zeros((8, LANES), i32) for _ in range(held)]
        whole = slots // 15
        carry = lax.fori_loop(
            0, whole, lambda g, carry: some(k, g * 15, 15, carry), (zero, list(zero))
        )
        if slots % 15:
            carry = some(k, whole * 15, slots % 15, carry)
        low, high = carry
        live = z_ref[slots + 3 : slots + 4, lane_tile(k)]
        for n in range(held):
            for field in range(8):
                part = low[n] if field % 2 == 0 else high[n]
                value = ((part >> (8 * (field // 2))) & 255).astype(f32) * live
                row = field * words + (n % per_tile) * 8
                outs[n // per_tile][row : row + 8, lane_tile(k)] = value
    for out in outs:
        out[cells : cells + FEATURES, :] = z_ref[slots : slots + FEATURES, :]


def own_counts_kernel(cells, own_ref, first_ref, mid_ref, second_ref, word_s, unit_s):
    count_source(1, own_ref, cells, (first_ref, mid_ref, second_ref), word_s, unit_s)


def counts_kernel(
    cells, first_ref, second_ref, own_first, own_mid, own_second, ltp_hbm,
    to_first, mid_ref, to_second, word_s, unit_s,
):
    outs = (to_first, mid_ref, to_second)
    for out, own in zip(outs, (own_first, own_mid, own_second)):
        out[1] = own[...]
    first, _, second = order("row")
    for q, source, z_ref in ((0, first, first_ref), (2, second, second_ref)):
        count_source(source, z_ref, cells, [out.at[q] for out in outs], word_s, unit_s)


def load_table(table_ref, ltp_s, par_s):
    cells = table_ref.shape[1]
    padded = ltp_s.shape[1]
    genes = table_ref.shape[0] - 8
    logs = [table_ref[0:genes, :]]
    if padded > genes:
        logs.append(jnp.zeros((padded - genes, cells), f32))
    rest = jnp.concatenate(logs, axis=0).T
    for part in range(PARTS):
        piece = rest.astype(bf16)
        ltp_s[part * cells : (part + 1) * cells, :] = piece
        if part + 1 < PARTS:
            rest = rest - piece.astype(f32)
    rows = [table_ref[genes : genes + 8, :], jnp.zeros((LANES - 8, cells), f32)]
    columns = jnp.concatenate(rows, axis=0).T
    for n in range(6):
        par_s[n] = jnp.broadcast_to(columns[:, n : n + 1], (cells, LANES))


def tables_kernel(first_ref, own_ref, second_ref, ltp_ref, par_ref):
    for side, table in enumerate((first_ref, own_ref, second_ref)):
        load_table(table, ltp_ref.at[side], par_ref.at[side])


def gene_hot(x_ref, source, cells, padded):
    tokens = x_ref.shape[2]
    gene = x_ref[source, cells + 2 : cells + 3, :].astype(i32).astype(jnp.int16)
    axis = lax.broadcasted_iota(jnp.int16, (padded, tokens), 0)
    return jnp.where(axis == gene, jnp.ones((), bf16), jnp.zeros((), bf16))


def features(x_ref, source, cells, row_step, col_step):
    y0 = x_ref[source, cells : cells + 1, :] + row_step
    y1 = x_ref[source, cells + 1 : cells + 2, :] + col_step
    return y0, y1


def score_rows(at, y0, y1, gl_s, par_s, cells):
    tiles = y0.shape[1] // LANES
    p = [jnp.concatenate([par_s[n, at : at + 8, :]] * tiles, axis=1) for n in range(6)]
    d0 = y0 - p[0]
    d1 = y1 - p[1]
    logs = gl_s[at : at + 8, :]
    for part in range(1, PARTS):
        logs = logs + gl_s[part * cells + at : part * cells + at + 8, :]
    return logs + p[5] + (d0 * (p[2] * d0 + p[3] * d1) + p[4] * d1 * d1)


def row_of(ref, index, first, tiles):
    return jnp.concatenate([ref[index + (pl.ds(first + k, 1), slice(None))] for k in range(tiles)], axis=1)


def to_tiles(row):
    return jnp.concatenate([row[:, k * LANES : (k + 1) * LANES] for k in range(row.shape[1] // LANES)], axis=0)


def log_sum(top, total):
    return jnp.where(total > 0.0, top + jnp.log(total), NEVER)


def joined(parts):
    top = functools.reduce(jnp.maximum, parts)
    return top + jnp.log(sum(jnp.exp(p - top) for p in parts))


def device_at(row_step, col_step):
    rows, cols = lax.axis_size("row"), lax.axis_size("col")
    row = lax.axis_index("row") + row_step
    col = lax.axis_index("col") + col_step
    inside = (row >= 0) & (row < rows) & (col >= 0) & (col < cols)
    return inside, jnp.clip(row, 0, rows - 1) * cols + jnp.clip(col, 0, cols - 1)


def send_first(part_s, out_ref):
    cols = lax.axis_size("col")
    row = lax.axis_index("row")
    tiles = part_s.shape[1]

    @pl.loop(0, out_ref.shape[0] // cols)
    def _(at):
        for q in range(3):
            source = at - row + q
            inside = (source >= 0) & (source < 3)
            part = jnp.where(inside, part_s[jnp.clip(source, 0, 2)], NEVER)
            for c in range(cols):
                out_ref[at * cols + c, q * tiles : (q + 1) * tiles, :] = part


def receive_first(in_ref, log_s):
    tiles = log_s.shape[2]
    for q in range(3):
        for s in range(3):
            parts = []
            for row_step in range(q - 2, q + 1):
                inside, at = device_at(row_step, s - 1)
                parts.append(jnp.where(inside, in_ref[at, q * tiles : (q + 1) * tiles, :], NEVER))
            log_s[q, s] = joined(parts)


def place(q, s, row_step, col_step):
    if row_step == 0:
        return q * 2 + s - max(0, -col_step)
    return (q - max(0, -row_step)) * 3 + s


def send_second(part_s, out_ref):
    tiles = part_s.shape[2]
    for row_step in range(-2, 3):
        for col_step in range(-2, 3):
            if row_step == 0 and col_step == 0:
                continue
            inside, at = device_at(row_step, col_step)

            @pl.when(inside)
            def _(row_step=row_step, col_step=col_step, at=at):
                for q in range(max(0, -row_step), min(3, 3 - row_step)):
                    for s in range(max(0, -col_step), min(3, 3 - col_step)):
                        slot = place(q, s, row_step, col_step) * tiles
                        out_ref[at, slot : slot + tiles, :] = part_s[q + row_step, s + col_step]


def receive_second(in_ref, own_ref, log_s):
    tiles = log_s.shape[2]
    for q in range(3):
        for s in range(3):
            parts = [own_ref[q, s]]
            for row_step in range(q - 2, q + 1):
                for col_step in range(s - 2, s + 1):
                    if row_step == 0 and col_step == 0:
                        continue
                    inside, at = device_at(row_step, col_step)
                    slot = place(q, s, -row_step, -col_step) * tiles
                    parts.append(jnp.where(inside, in_ref[at, slot : slot + tiles, :], NEVER))
            log_s[q, s] = joined(parts)


def row_parts_kernel(
    first_ref, mid_ref, second_ref, ltp_s, par_s, out_ref, part_s, gl_s, sc_s
):
    x_refs = (first_ref, mid_ref, second_ref)
    cells, tokens = sc_s.shape[1:]

    for q, source in enumerate(order("row")):
        hot = gene_hot(mid_ref, q, cells, ltp_s.shape[2])
        for side in range(3):
            gl_s[side] = jnp.dot(ltp_s[side], hot, preferred_element_type=f32)
        top = jnp.full((8, tokens), NEVER, f32)
        for side, at_side in enumerate(order("col")):
            y0, y1 = features(mid_ref, q, cells, as_float(source) - 1.0, 1.0 - as_float(at_side))
            for at in range(0, cells, 8):
                score = score_rows(at, y0, y1, gl_s.at[side], par_s.at[side], cells)
                score = jnp.where(x_refs[side][q, at : at + 8, :] > 0.0, score, NEVER)
                sc_s[side, at : at + 8, :] = score
                top = jnp.maximum(top, score)
        top = jnp.max(top, axis=0, keepdims=True)
        total = jnp.zeros((8, tokens), f32)
        for side in range(3):
            for at in range(0, cells, 8):
                count = x_refs[side][q, at : at + 8, :]
                total = total + count * jnp.exp(sc_s[side, at : at + 8, :] - top)
        total = jnp.sum(total, axis=0, keepdims=True)
        part_s[source] = to_tiles(log_sum(top, total))
    send_first(part_s, out_ref)


def add_moments(p, y0, y1, sums):
    def fold(x):
        parts = [x[:, k * LANES : (k + 1) * LANES] for k in range(x.shape[1] // LANES)]
        return functools.reduce(jnp.add, parts)

    weights = (None, y0, y1, y0 * y0, y0 * y1, y1 * y1)
    return [s + fold(p if w is None else p * w) for s, w in zip(sums, weights)]


def add_counts(hot, sh_s, cnt_s):
    cnt_s[...] += lax.dot_general(hot, sh_s[...], (((1,), (1,)), ((), ())), preferred_element_type=f32)


def new_cells(genes, mom_s, cnt_s, state_ref):
    weight, s0, s1, s00, s01, s11 = [jnp.sum(mom_s[n].T, axis=0, keepdims=True) for n in range(6)]
    mu_row, mu_col, rr, rc, cc = [state_ref[n : n + 1, :] for n in range(5)]
    counts = cnt_s[0:genes, :]
    profile = (counts + pseudo_count) / (
        jnp.sum(counts, axis=0, keepdims=True) + genes * pseudo_count
    )
    denominator = weight + prior_weight
    new_row = (s0 + prior_weight * mu_row) / denominator
    new_col = (s1 + prior_weight * mu_col) / denominator
    q_rr = s00 - 2.0 * new_row * s0 + weight * new_row * new_row
    q_rc = s01 - new_row * s1 - new_col * s0 + weight * new_row * new_col
    q_cc = s11 - 2.0 * new_col * s1 + weight * new_col * new_col
    state = (
        new_row,
        new_col,
        (q_rr + prior_weight * rr) / denominator,
        (q_rc + prior_weight * rc) / denominator,
        (q_cc + prior_weight * cc) / denominator,
    )
    return profile, state, jnp.log(weight + 1.0)


def middle_kernel(
    genes,
    first_ref, mid_ref, second_ref, ltp_ref, par_ref, state_ref, told_ref,
    e_ref, m_ref, part_ref, out_ref, state_out,
    hot_s, sh_s, mom_s, cnt_s, ltp_s, par_s, gl_s, sc_s, table_s, log_s,
):
    x_refs = (first_ref, mid_ref, second_ref)
    cells, tokens = sc_s.shape[1:]
    tiles = tokens // LANES
    padded = cnt_s.shape[0]
    mom_s[...] = jnp.zeros(mom_s.shape, f32)
    cnt_s[...] = jnp.zeros(cnt_s.shape, f32)
    receive_first(told_ref, log_s)

    for q, source in enumerate(order("row")):
        for side, x_ref in enumerate(x_refs):
            hot_s[q, side] = gene_hot(x_ref, q, cells, padded)
            gl_s[side] = jnp.dot(ltp_ref[1], hot_s[q, side], preferred_element_type=f32)
        for side, (at_side, x_ref) in enumerate(zip(order("col"), x_refs)):
            total = row_of(log_s, (source, at_side), 0, tiles)
            y0, y1 = features(x_ref, q, cells, as_float(source) - 1.0, as_float(at_side) - 1.0)
            for at in range(0, cells, 16):
                halves = []
                for a in (at, at + 8):
                    score = score_rows(a, y0, y1, gl_s.at[side], par_ref.at[1], cells)
                    count = x_ref[q, a : a + 8, :]
                    p = count * jnp.exp(jnp.minimum(score - total, 0.0))
                    sums = [mom_s[n, a : a + 8, :] for n in range(6)]
                    sums = add_moments(p, y0, y1, sums)
                    for n in range(6):
                        mom_s[n, a : a + 8, :] = sums[n]
                    halves.append(p)
                sh_s[side, at : at + 16, :] = jnp.concatenate(halves, axis=0).astype(bf16)
            add_counts(hot_s[q, side], sh_s.at[side], cnt_s)

    profile, state, log_weight = new_cells(genes, mom_s, cnt_s, state_ref)
    state_out[...] = state_rows(state)
    table_s[...] = table_rows(profile, state, log_weight)
    load_table(table_s, ltp_s, par_s)

    for q, source in enumerate(order("row")):
        for side in range(3):
            gl_s[side] = jnp.dot(ltp_s[...], hot_s[q, side], preferred_element_type=f32)
        for side, (at_side, x_ref) in enumerate(zip(order("col"), x_refs)):
            y0, y1 = features(x_ref, q, cells, as_float(source) - 1.0, as_float(at_side) - 1.0)
            top = jnp.full((8, tokens), NEVER, f32)
            for at in range(0, cells, 8):
                value = score_rows(at, y0, y1, gl_s.at[side], par_s, cells)
                value = jnp.where(x_ref[q, at : at + 8, :] > 0.0, value, NEVER)
                sc_s[side, at : at + 8, :] = value
                top = jnp.maximum(top, value)
            top = jnp.max(top, axis=0, keepdims=True)
            total = jnp.zeros((8, tokens), f32)
            for at in range(0, cells, 8):
                e = x_ref[q, at : at + 8, :] * jnp.exp(sc_s[side, at : at + 8, :] - top)
                e_ref[q, side, at : at + 8, :] = e
                total = total + e
            total = jnp.sum(total, axis=0, keepdims=True)
            m_ref[source, at_side] = to_tiles(top)
            part_ref[source, at_side] = to_tiles(log_sum(top, total))

    send_second(part_ref, out_ref)


def last_kernel(
    genes,
    first_ref, mid_ref, second_ref, e_ref, m_ref, part_ref, told_ref, state_ref,
    profile_ref, cells_ref,
    sh_s, mom_s, cnt_s, log_s,
):
    x_refs = (first_ref, mid_ref, second_ref)
    cells, tokens = sh_s.shape[1:]
    tiles = tokens // LANES
    mom_s[...] = jnp.zeros(mom_s.shape, f32)
    cnt_s[...] = jnp.zeros(cnt_s.shape, f32)
    receive_second(told_ref, part_ref, log_s)

    for q, source in enumerate(order("row")):
        for side, (at_side, x_ref) in enumerate(zip(order("col"), x_refs)):
            scale = jnp.exp(m_ref[source, at_side] - log_s[source, at_side])
            factor = jnp.concatenate([scale[k : k + 1, :] for k in range(tiles)], axis=1)
            y0, y1 = features(x_ref, q, cells, as_float(source) - 1.0, as_float(at_side) - 1.0)
            for at in range(0, cells, 16):
                halves = []
                for a in (at, at + 8):
                    p = e_ref[q, side, a : a + 8, :] * factor
                    sums = [mom_s[n, a : a + 8, :] for n in range(6)]
                    sums = add_moments(p, y0, y1, sums)
                    for n in range(6):
                        mom_s[n, a : a + 8, :] = sums[n]
                    halves.append(p)
                sh_s[side, at : at + 16, :] = jnp.concatenate(halves, axis=0).astype(bf16)
            add_counts(gene_hot(x_ref, q, cells, cnt_s.shape[0]), sh_s.at[side], cnt_s)

    profile, state, log_weight = new_cells(genes, mom_s, cnt_s, state_ref)
    profile_ref[...] = jnp.log(profile)
    mu_row, mu_col, rr, rc, cc = state
    final = (mu_row, mu_col, 0.5 * jnp.log(rr), 0.5 * jnp.log(cc), rc / jnp.sqrt(rr * cc), log_weight)
    for n, row in enumerate(final):
        cells_ref[n] = row


def body(
    positions, genes, candidates, block_counts, profile_weights, centroids, spreads, correlation
):
    gene_total = profile_weights.shape[0]
    cells = profile_weights.shape[3]
    tokens, slots = candidates.shape[2:]
    tiles = tokens // LANES
    group = lax.axis_size("row") * lax.axis_size("col")
    padded = padded_to(gene_total, LANES)
    pairs = 9 * tokens * cells
    table = ((padded_to(gene_total, 8) + 8, cells), f32)
    state = ((8, cells), f32)
    vmem = pltpu.VMEM

    packed, table_own, state_own = call(
        pack_kernel, "pack", [((slots + FEATURES, tokens), f32), table, state],
        [ANY] * 8,
        [
            vmem((1, block_counts.shape[2]), i32),
            vmem((tokens, slots), i32),
            vmem((2 * tiles, LANES), f32),
            vmem((tiles, LANES), i32),
            vmem((gene_total, cells), f32),
            vmem((2, cells), f32),
            vmem((2, cells), f32),
            vmem((1, cells), f32),
            pltpu.SemaphoreType.DMA((8,)),
        ],
        tokens * slots,
        [
            pltpu.with_memory_space_constraint(a, pltpu.HBM)
            for a in (
                block_counts.reshape(1, -1),
                candidates.reshape(tokens, slots),
                positions.reshape(2 * tiles, LANES),
                genes.reshape(tiles, LANES),
                profile_weights.reshape(gene_total, cells),
                centroids.reshape(2, cells),
                spreads.reshape(2, cells),
                correlation.reshape(1, cells),
            )
        ],
    )
    row_first, row_second = swapped(packed, packed, "row")
    table_first, table_second = swapped(table_own, table_own, "col")
    ltp, par = call(
        tables_kernel, "tables",
        [((3, PARTS * cells, padded), bf16), ((3, 6, cells, LANES), f32)], [VMEM] * 3, [],
        tokens * slots, (table_first, table_own, table_second),
    )
    one = ((cells + FEATURES, tokens), f32)
    three = ((3, cells + FEATURES, tokens), f32)
    count_scratch = [vmem((tiles, slots + 8, LANES), i32)] * 2
    own = call(
        functools.partial(own_counts_kernel, cells), "own_counts", [one] * 3, [VMEM],
        count_scratch, pairs * 40, (packed,),
    )
    to_first, mid, to_second = call(
        functools.partial(counts_kernel, cells), "counts", [three] * 3, [VMEM] * 5 + [ANY],
        count_scratch, pairs * 80, (row_first, row_second, *own, ltp),
    )
    from_first, from_second = swapped(to_first, to_second, "col")

    logs = (tiles, LANES)
    parts, = call(
        row_parts_kernel, "row_parts", [((group, padded_to(3 * tiles, 8), LANES), f32)], [VMEM] * 5,
        [
            vmem((3,) + logs, f32),
            vmem((3, PARTS * cells, tokens), f32),
            vmem((3, cells, tokens), f32),
        ],
        pairs * 100,
        (to_first, mid, to_second, ltp, par),
    )
    told = lax.all_to_all(parts, ("row", "col"), 0, 0)

    x = (from_first, mid, from_second)
    sum_scratch = [
        vmem((3, cells, tokens), bf16),
        vmem((6, cells, LANES), f32),
        vmem((padded, cells), f32),
    ]
    e, m, held, parts, state_own = call(
        functools.partial(middle_kernel, gene_total), "middle",
        [
            ((3, 3, cells, tokens), f32),
            ((3, 3) + logs, f32),
            ((3, 3) + logs, f32),
            ((group, 6 * tiles, LANES), f32),
            state,
        ],
        [VMEM] * 7,
        [vmem((3, 3, padded, tokens), bf16)] + sum_scratch + [
            vmem((PARTS * cells, padded), bf16),
            vmem((6, cells, LANES), f32),
            vmem((3, PARTS * cells, tokens), f32),
            vmem((3, cells, tokens), f32),
            vmem(*table),
            vmem((3, 3) + logs, f32),
        ],
        pairs * 200,
        (*x, ltp, par, state_own, told),
    )
    told = lax.all_to_all(parts, ("row", "col"), 0, 0)
    final_profile, final_cells = call(
        functools.partial(last_kernel, gene_total), "last",
        [((gene_total, cells), f32), ((6, 1, cells), f32)],
        [VMEM] * 8, sum_scratch + [vmem((3, 3) + logs, f32)], pairs * 100,
        (*x, e, m, held, told, state_own),
    )
    return (final_profile.reshape(gene_total, 1, 1, cells), final_cells.reshape(6, 1, 1, cells))


def solution(mesh):
    tiles = P(("groups", "row"), "col")
    stacked = P(None, ("groups", "row"), "col", None)
    return jax.shard_map(
        body,
        mesh=mesh,
        in_specs=(
            stacked,
            P(("groups", "row"), "col", None),
            P(("groups", "row"), "col", None, None),
            P(("groups", "row"), "col", None),
            stacked,
            stacked,
            stacked,
            P(("groups", "row"), "col", None),
        ),
        out_specs=(stacked, stacked),
        check_vma=False,
    )
```

```python
import functools

import jax
import jax.numpy as jnp
from jax import lax
from jax.experimental import pallas as pl
from jax.experimental.pallas import tpu as pltpu
from jax.sharding import PartitionSpec as P

BLOCK = 256
LANES = 128
FEATURES = 8
PARTS = 2
NEVER = -1e30

pseudo_count = 0.05
prior_weight = 1.0

f32 = jnp.float32
bf16 = jnp.bfloat16
i32 = jnp.int32


def swapped(to_first, to_second, axis):
    count = lax.axis_size(axis)
    out = []
    for start, x in enumerate((to_first, to_second)):
        pairs = [p for i in range(start, count - 1, 2) for p in ((i, i + 1), (i + 1, i))]
        out.append(lax.ppermute(x, axis, pairs))
    return out


def params(mib=40):
    return pltpu.CompilerParams(vmem_limit_bytes=mib << 20)


def cost(flops, size):
    return pl.CostEstimate(flops=flops, bytes_accessed=size, transcendentals=0)


def call(kernel, name, outs, in_specs, scratch, flops, args):
    shapes = [jax.ShapeDtypeStruct(s, d) for s, d in outs]
    return pl.pallas_call(
        kernel,
        name=name,
        out_shape=shapes,
        in_specs=in_specs,
        out_specs=[pl.BlockSpec(memory_space=pltpu.VMEM)] * len(shapes),
        scratch_shapes=scratch,
        compiler_params=params(),
        cost_estimate=cost(flops, 1 << 20),
    )(*args)


VMEM = pl.BlockSpec(memory_space=pltpu.VMEM)
SMEM = pl.BlockSpec(memory_space=pltpu.SMEM)
ANY = pl.BlockSpec(memory_space=pltpu.HBM)


def lane_tile(k):
    return pl.ds(k * LANES, LANES)


def padded_to(size, unit):
    return -(-size // unit) * unit


def order(axis):
    first = 2 * (1 - lax.rem(lax.axis_index(axis), 2))
    return (first, 1, 2 - first)


def as_float(x):
    return x.astype(f32) if hasattr(x, "astype") else float(x)


def table_rows(profile, state, log_weight):
    genes, cells = profile.shape
    mu_row, mu_col, rr, rc, cc = state
    det = rr * cc - rc * rc
    rows = [jnp.log(profile)]
    if genes % 8:
        rows.append(jnp.zeros((-genes % 8, cells), f32))
    rows += [
        mu_row,
        mu_col,
        -0.5 * (cc / det),
        rc / det,
        -0.5 * (rr / det),
        log_weight - 0.5 * jnp.log(det),
        jnp.zeros((2, cells), f32),
    ]
    return jnp.concatenate(rows, axis=0)


def state_rows(state):
    return jnp.concatenate(list(state) + [jnp.zeros((3, state[0].shape[1]), f32)], axis=0)


def pack_kernel(
    count_hbm, cand_hbm, pos_hbm, gene_hbm, weight_hbm, centre_hbm, spread_hbm, corr_hbm,
    out_ref, table_ref, state_ref,
    count_ref, cand_ref, pos_ref, gene_ref, weight_ref, centre_ref, spread_ref, corr_ref, sems,
):
    pairs = (
        (count_hbm, count_ref), (cand_hbm, cand_ref), (pos_hbm, pos_ref), (gene_hbm, gene_ref), (weight_hbm, weight_ref),
        (centre_hbm, centre_ref), (spread_hbm, spread_ref), (corr_hbm, corr_ref),
    )
    copies = [pltpu.make_async_copy(a, b, sems.at[n]) for n, (a, b) in enumerate(pairs)]
    for copy in copies:
        copy.start()
    for copy in copies[:4]:
        copy.wait()
    tokens, slots = cand_ref.shape
    tiles = tokens // LANES
    out_ref[0:slots, :] = cand_ref[...].astype(f32).T
    lane = lax.broadcasted_iota(i32, (1, LANES), 1)
    for k in range(tiles):
        start = k * LANES
        live = (start % BLOCK + lane) < count_ref[:, start // BLOCK : start // BLOCK + 1]
        rows = [
            pos_ref[k : k + 1, :],
            pos_ref[tiles + k : tiles + k + 1, :],
            gene_ref[k : k + 1, :].astype(f32),
            live.astype(f32),
            jnp.zeros((FEATURES - 4, LANES), f32),
        ]
        out_ref[slots : slots + FEATURES, lane_tile(k)] = jnp.concatenate(rows, axis=0)
    for copy in copies[4:]:
        copy.wait()
    weights = weight_ref[...]
    spread_row, spread_col = spread_ref[0:1, :], spread_ref[1:2, :]
    state = (
        centre_ref[0:1, :],
        centre_ref[1:2, :],
        spread_row * spread_row,
        corr_ref[0:1, :] * spread_row * spread_col,
        spread_col * spread_col,
    )
    state_ref[...] = state_rows(state)
    profile = weights / jnp.sum(weights, axis=0, keepdims=True)
    table_ref[...] = table_rows(profile, state, jnp.zeros_like(spread_row))


def full_add(a, b, c):
    both = a ^ b
    return both ^ c, (a & b) | (both & c)


def count_source(source, z_ref, cells, outs, word_s, unit_s):
    rows, tokens = z_ref.shape
    slots = rows - FEATURES
    shift = cells.bit_length() - 1
    held = cells // 64
    planes = slots.bit_length()
    sub = lax.broadcasted_iota(i32, (8, LANES), 0)
    first = order("col")[0]
    for k in range(tokens // LANES):
        local = z_ref[0:slots, lane_tile(k)].astype(i32) - (2 - source) * 3 * cells
        tile = first + (local >> shift) * (1 - first)
        cell = local & (cells - 1)
        live = z_ref[slots + 3 : slots + 4, lane_tile(k)] > 0.0
        named = (tile >= 0) & (tile < 3) & live
        word_s[k, 0:slots, :] = ((cell >> 6) << 3) | (cell & 7)
        unit_s[k, 0:slots, :] = jnp.where(named, 1 << (((tile & 3) << 3) | ((cell >> 3) & 7)), 0)

    for k in range(tokens // LANES):

        def group(g, carry):
            bits = [[] for _ in range(held)]
            for j in range(16):
                which = word_s[k, pl.ds(g * 16 + j, 8, stride=0), :]
                unit = unit_s[k, pl.ds(g * 16 + j, 8, stride=0), :]
                for n in range(held):
                    bits[n].append(jnp.where(which == sub + 8 * n, unit, 0))
            out = []
            for n in range(held):
                plane = list(carry[n])
                level = bits[n]
                for p in range(4):
                    following = []
                    for a in range(0, len(level), 2):
                        plane[p], over = full_add(plane[p], level[a], level[a + 1])
                        following.append(over)
                    level = following
                over = level[0]
                for p in range(4, planes):
                    plane[p], over = plane[p] ^ over, plane[p] & over
                out.append(plane)
            return out

        zero = jnp.zeros((8, LANES), i32)
        total = lax.fori_loop(0, slots // 16, group, [[zero] * planes for _ in range(held)], unroll=True)
        for n in range(held):
            for r in range(8):
                value = zero
                for p in range(planes):
                    moved = total[n][p]
                    if r > p:
                        moved = moved >> (r - p)
                    elif r < p:
                        moved = moved << (p - r)
                    value = value | (moved & (0x00010101 << p))
                row = n * 64 + r * 8
                for tile, out in enumerate(outs):
                    part = value & 255 if tile == 0 else (value >> (8 * tile)) & 255
                    out[row : row + 8, lane_tile(k)] = part.astype(f32)
    for out in outs:
        out[cells : cells + FEATURES, :] = z_ref[slots : slots + FEATURES, :]


def own_counts_kernel(cells, own_ref, first_ref, mid_ref, second_ref, word_s, unit_s):
    count_source(1, own_ref, cells, (first_ref, mid_ref, second_ref), word_s, unit_s)


def counts_kernel(
    cells, first_ref, second_ref, own_first, own_mid, own_second, ltp_hbm,
    to_first, mid_ref, to_second, word_s, unit_s,
):
    outs = (to_first, mid_ref, to_second)
    for out, own in zip(outs, (own_first, own_mid, own_second)):
        out[1] = own[...]
    first, _, second = order("row")
    for q, source, z_ref in ((0, first, first_ref), (2, second, second_ref)):
        count_source(source, z_ref, cells, [out.at[q] for out in outs], word_s, unit_s)


def load_table(table_ref, ltp_s, par_s):
    cells = table_ref.shape[1]
    padded = ltp_s.shape[1]
    genes = table_ref.shape[0] - 8
    logs = [table_ref[0:genes, :]]
    if padded > genes:
        logs.append(jnp.zeros((padded - genes, cells), f32))
    rest = jnp.concatenate(logs, axis=0).T
    for part in range(PARTS):
        piece = rest.astype(bf16)
        ltp_s[part * cells : (part + 1) * cells, :] = piece
        if part + 1 < PARTS:
            rest = rest - piece.astype(f32)
    rows = [table_ref[genes : genes + 8, :], jnp.zeros((LANES - 8, cells), f32)]
    columns = jnp.concatenate(rows, axis=0).T
    for n in range(6):
        par_s[n] = jnp.broadcast_to(columns[:, n : n + 1], (cells, LANES))


def tables_kernel(first_ref, own_ref, second_ref, ltp_ref, par_ref):
    for side, table in enumerate((first_ref, own_ref, second_ref)):
        load_table(table, ltp_ref.at[side], par_ref.at[side])


def gene_hot(x_ref, source, cells, padded):
    tokens = x_ref.shape[2]
    gene = x_ref[source, cells + 2 : cells + 3, :].astype(i32).astype(jnp.int16)
    axis = lax.broadcasted_iota(jnp.int16, (padded, tokens), 0)
    return jnp.where(axis == gene, jnp.ones((), bf16), jnp.zeros((), bf16))


def features(x_ref, source, cells, row_step, col_step):
    y0 = x_ref[source, cells : cells + 1, :] + row_step
    y1 = x_ref[source, cells + 1 : cells + 2, :] + col_step
    return y0, y1


def score_rows(at, y0, y1, gl_s, par_s, cells):
    tiles = y0.shape[1] // LANES
    p = [jnp.concatenate([par_s[n, at : at + 8, :]] * tiles, axis=1) for n in range(6)]
    d0 = y0 - p[0]
    d1 = y1 - p[1]
    logs = gl_s[at : at + 8, :]
    for part in range(1, PARTS):
        logs = logs + gl_s[part * cells + at : part * cells + at + 8, :]
    return logs + p[5] + (d0 * (p[2] * d0 + p[3] * d1) + p[4] * d1 * d1)


def row_of(ref, index, first, tiles):
    return jnp.concatenate([ref[index + (pl.ds(first + k, 1), slice(None))] for k in range(tiles)], axis=1)


def to_tiles(row):
    return jnp.concatenate([row[:, k * LANES : (k + 1) * LANES] for k in range(row.shape[1] // LANES)], axis=0)


def log_sum(top, total):
    return jnp.where(total > 0.0, top + jnp.log(total), NEVER)


def joined(parts):
    top = functools.reduce(jnp.maximum, parts)
    return top + jnp.log(sum(jnp.exp(p - top) for p in parts))


def device_at(row_step, col_step):
    rows, cols = lax.axis_size("row"), lax.axis_size("col")
    row = lax.axis_index("row") + row_step
    col = lax.axis_index("col") + col_step
    inside = (row >= 0) & (row < rows) & (col >= 0) & (col < cols)
    return inside, jnp.clip(row, 0, rows - 1) * cols + jnp.clip(col, 0, cols - 1)


def send_first(part_s, out_ref):
    cols = lax.axis_size("col")
    row = lax.axis_index("row")
    tiles = part_s.shape[1]

    @pl.loop(0, out_ref.shape[0] // cols)
    def _(at):
        for q in range(3):
            source = at - row + q
            inside = (source >= 0) & (source < 3)
            part = jnp.where(inside, part_s[jnp.clip(source, 0, 2)], NEVER)
            for c in range(cols):
                out_ref[at * cols + c, q * tiles : (q + 1) * tiles, :] = part


def receive_first(in_ref, log_s):
    tiles = log_s.shape[2]
    for q in range(3):
        for s in range(3):
            parts = []
            for row_step in range(q - 2, q + 1):
                inside, at = device_at(row_step, s - 1)
                parts.append(jnp.where(inside, in_ref[at, q * tiles : (q + 1) * tiles, :], NEVER))
            log_s[q, s] = joined(parts)


def place(q, s, row_step, col_step):
    if row_step == 0:
        return q * 2 + s - max(0, -col_step)
    return (q - max(0, -row_step)) * 3 + s


def send_second(part_s, out_ref):
    tiles = part_s.shape[2]
    for row_step in range(-2, 3):
        for col_step in range(-2, 3):
            if row_step == 0 and col_step == 0:
                continue
            inside, at = device_at(row_step, col_step)

            @pl.when(inside)
            def _(row_step=row_step, col_step=col_step, at=at):
                for q in range(max(0, -row_step), min(3, 3 - row_step)):
                    for s in range(max(0, -col_step), min(3, 3 - col_step)):
                        slot = place(q, s, row_step, col_step) * tiles
                        out_ref[at, slot : slot + tiles, :] = part_s[q + row_step, s + col_step]


def receive_second(in_ref, own_ref, log_s):
    tiles = log_s.shape[2]
    for q in range(3):
        for s in range(3):
            parts = [own_ref[q, s]]
            for row_step in range(q - 2, q + 1):
                for col_step in range(s - 2, s + 1):
                    if row_step == 0 and col_step == 0:
                        continue
                    inside, at = device_at(row_step, col_step)
                    slot = place(q, s, -row_step, -col_step) * tiles
                    parts.append(jnp.where(inside, in_ref[at, slot : slot + tiles, :], NEVER))
            log_s[q, s] = joined(parts)


def row_parts_kernel(
    first_ref, mid_ref, second_ref, ltp_s, par_s, out_ref, part_s, gl_s, sc_s
):
    x_refs = (first_ref, mid_ref, second_ref)
    cells, tokens = sc_s.shape[1:]

    for q, source in enumerate(order("row")):
        hot = gene_hot(mid_ref, q, cells, ltp_s.shape[2])
        for side in range(3):
            gl_s[side] = jnp.dot(ltp_s[side], hot, preferred_element_type=f32)
        top = jnp.full((8, tokens), NEVER, f32)
        for side, at_side in enumerate(order("col")):
            y0, y1 = features(mid_ref, q, cells, as_float(source) - 1.0, 1.0 - as_float(at_side))
            for at in range(0, cells, 8):
                score = score_rows(at, y0, y1, gl_s.at[side], par_s.at[side], cells)
                score = jnp.where(x_refs[side][q, at : at + 8, :] > 0.0, score, NEVER)
                sc_s[side, at : at + 8, :] = score
                top = jnp.maximum(top, score)
        top = jnp.max(top, axis=0, keepdims=True)
        total = jnp.zeros((8, tokens), f32)
        for side in range(3):
            for at in range(0, cells, 8):
                count = x_refs[side][q, at : at + 8, :]
                total = total + count * jnp.exp(sc_s[side, at : at + 8, :] - top)
        total = jnp.sum(total, axis=0, keepdims=True)
        part_s[source] = to_tiles(log_sum(top, total))
    send_first(part_s, out_ref)


def add_moments(p, y0, y1, sums):
    def fold(x):
        parts = [x[:, k * LANES : (k + 1) * LANES] for k in range(x.shape[1] // LANES)]
        return functools.reduce(jnp.add, parts)

    weights = (None, y0, y1, y0 * y0, y0 * y1, y1 * y1)
    return [s + fold(p if w is None else p * w) for s, w in zip(sums, weights)]


def add_counts(hot, sh_s, cnt_s):
    cnt_s[...] += lax.dot_general(hot, sh_s[...], (((1,), (1,)), ((), ())), preferred_element_type=f32)


def new_cells(genes, mom_s, cnt_s, state_ref):
    weight, s0, s1, s00, s01, s11 = [jnp.sum(mom_s[n].T, axis=0, keepdims=True) for n in range(6)]
    mu_row, mu_col, rr, rc, cc = [state_ref[n : n + 1, :] for n in range(5)]
    counts = cnt_s[0:genes, :]
    profile = (counts + pseudo_count) / (
        jnp.sum(counts, axis=0, keepdims=True) + genes * pseudo_count
    )
    denominator = weight + prior_weight
    new_row = (s0 + prior_weight * mu_row) / denominator
    new_col = (s1 + prior_weight * mu_col) / denominator
    q_rr = s00 - 2.0 * new_row * s0 + weight * new_row * new_row
    q_rc = s01 - new_row * s1 - new_col * s0 + weight * new_row * new_col
    q_cc = s11 - 2.0 * new_col * s1 + weight * new_col * new_col
    state = (
        new_row,
        new_col,
        (q_rr + prior_weight * rr) / denominator,
        (q_rc + prior_weight * rc) / denominator,
        (q_cc + prior_weight * cc) / denominator,
    )
    return profile, state, jnp.log(weight + 1.0)


def middle_kernel(
    genes,
    first_ref, mid_ref, second_ref, ltp_ref, par_ref, state_ref, told_ref,
    e_ref, m_ref, part_ref, out_ref, state_out,
    hot_s, sh_s, mom_s, cnt_s, ltp_s, par_s, gl_s, sc_s, table_s, log_s,
):
    x_refs = (first_ref, mid_ref, second_ref)
    cells, tokens = sc_s.shape[1:]
    tiles = tokens // LANES
    padded = cnt_s.shape[0]
    mom_s[...] = jnp.zeros(mom_s.shape, f32)
    cnt_s[...] = jnp.zeros(cnt_s.shape, f32)
    receive_first(told_ref, log_s)

    for q, source in enumerate(order("row")):
        for side, x_ref in enumerate(x_refs):
            hot_s[q, side] = gene_hot(x_ref, q, cells, padded)
            gl_s[side] = jnp.dot(ltp_ref[1], hot_s[q, side], preferred_element_type=f32)
        for side, (at_side, x_ref) in enumerate(zip(order("col"), x_refs)):
            total = row_of(log_s, (source, at_side), 0, tiles)
            y0, y1 = features(x_ref, q, cells, as_float(source) - 1.0, as_float(at_side) - 1.0)
            for at in range(0, cells, 16):
                halves = []
                for a in (at, at + 8):
                    score = score_rows(a, y0, y1, gl_s.at[side], par_ref.at[1], cells)
                    count = x_ref[q, a : a + 8, :]
                    p = count * jnp.exp(jnp.minimum(score - total, 0.0))
                    sums = [mom_s[n, a : a + 8, :] for n in range(6)]
                    sums = add_moments(p, y0, y1, sums)
                    for n in range(6):
                        mom_s[n, a : a + 8, :] = sums[n]
                    halves.append(p)
                sh_s[side, at : at + 16, :] = jnp.concatenate(halves, axis=0).astype(bf16)
            add_counts(hot_s[q, side], sh_s.at[side], cnt_s)

    profile, state, log_weight = new_cells(genes, mom_s, cnt_s, state_ref)
    state_out[...] = state_rows(state)
    table_s[...] = table_rows(profile, state, log_weight)
    load_table(table_s, ltp_s, par_s)

    for q, source in enumerate(order("row")):
        for side in range(3):
            gl_s[side] = jnp.dot(ltp_s[...], hot_s[q, side], preferred_element_type=f32)
        for side, (at_side, x_ref) in enumerate(zip(order("col"), x_refs)):
            y0, y1 = features(x_ref, q, cells, as_float(source) - 1.0, as_float(at_side) - 1.0)
            top = jnp.full((8, tokens), NEVER, f32)
            for at in range(0, cells, 8):
                value = score_rows(at, y0, y1, gl_s.at[side], par_s, cells)
                value = jnp.where(x_ref[q, at : at + 8, :] > 0.0, value, NEVER)
                sc_s[side, at : at + 8, :] = value
                top = jnp.maximum(top, value)
            top = jnp.max(top, axis=0, keepdims=True)
            total = jnp.zeros((8, tokens), f32)
            for at in range(0, cells, 8):
                e = x_ref[q, at : at + 8, :] * jnp.exp(sc_s[side, at : at + 8, :] - top)
                e_ref[q, side, at : at + 8, :] = e
                total = total + e
            total = jnp.sum(total, axis=0, keepdims=True)
            m_ref[source, at_side] = to_tiles(top)
            part_ref[source, at_side] = to_tiles(log_sum(top, total))

    send_second(part_ref, out_ref)


def last_kernel(
    genes,
    first_ref, mid_ref, second_ref, e_ref, m_ref, part_ref, told_ref, state_ref,
    profile_ref, cells_ref,
    sh_s, mom_s, cnt_s, log_s,
):
    x_refs = (first_ref, mid_ref, second_ref)
    cells, tokens = sh_s.shape[1:]
    tiles = tokens // LANES
    mom_s[...] = jnp.zeros(mom_s.shape, f32)
    cnt_s[...] = jnp.zeros(cnt_s.shape, f32)
    receive_second(told_ref, part_ref, log_s)

    for q, source in enumerate(order("row")):
        for side, (at_side, x_ref) in enumerate(zip(order("col"), x_refs)):
            scale = jnp.exp(m_ref[source, at_side] - log_s[source, at_side])
            factor = jnp.concatenate([scale[k : k + 1, :] for k in range(tiles)], axis=1)
            y0, y1 = features(x_ref, q, cells, as_float(source) - 1.0, as_float(at_side) - 1.0)
            for at in range(0, cells, 16):
                halves = []
                for a in (at, at + 8):
                    p = e_ref[q, side, a : a + 8, :] * factor
                    sums = [mom_s[n, a : a + 8, :] for n in range(6)]
                    sums = add_moments(p, y0, y1, sums)
                    for n in range(6):
                        mom_s[n, a : a + 8, :] = sums[n]
                    halves.append(p)
                sh_s[side, at : at + 16, :] = jnp.concatenate(halves, axis=0).astype(bf16)
            add_counts(gene_hot(x_ref, q, cells, cnt_s.shape[0]), sh_s.at[side], cnt_s)

    profile, state, log_weight = new_cells(genes, mom_s, cnt_s, state_ref)
    profile_ref[...] = jnp.log(profile)
    mu_row, mu_col, rr, rc, cc = state
    final = (mu_row, mu_col, 0.5 * jnp.log(rr), 0.5 * jnp.log(cc), rc / jnp.sqrt(rr * cc), log_weight)
    for n, row in enumerate(final):
        cells_ref[n] = row


def body(
    positions, genes, candidates, block_counts, profile_weights, centroids, spreads, correlation
):
    gene_total = profile_weights.shape[0]
    cells = profile_weights.shape[3]
    tokens, slots = candidates.shape[2:]
    tiles = tokens // LANES
    group = lax.axis_size("row") * lax.axis_size("col")
    padded = padded_to(gene_total, LANES)
    pairs = 9 * tokens * cells
    table = ((padded_to(gene_total, 8) + 8, cells), f32)
    state = ((8, cells), f32)
    vmem = pltpu.VMEM

    packed, table_own, state_own = call(
        pack_kernel, "pack", [((slots + FEATURES, tokens), f32), table, state],
        [ANY] * 8,
        [
            vmem((1, block_counts.shape[2]), i32),
            vmem((tokens, slots), i32),
            vmem((2 * tiles, LANES), f32),
            vmem((tiles, LANES), i32),
            vmem((gene_total, cells), f32),
            vmem((2, cells), f32),
            vmem((2, cells), f32),
            vmem((1, cells), f32),
            pltpu.SemaphoreType.DMA((8,)),
        ],
        tokens * slots,
        [
            pltpu.with_memory_space_constraint(a, pltpu.HBM)
            for a in (
                block_counts.reshape(1, -1),
                candidates.reshape(tokens, slots),
                positions.reshape(2 * tiles, LANES),
                genes.reshape(tiles, LANES),
                profile_weights.reshape(gene_total, cells),
                centroids.reshape(2, cells),
                spreads.reshape(2, cells),
                correlation.reshape(1, cells),
            )
        ],
    )
    row_first, row_second = swapped(packed, packed, "row")
    table_first, table_second = swapped(table_own, table_own, "col")
    ltp, par = call(
        tables_kernel, "tables",
        [((3, PARTS * cells, padded), bf16), ((3, 6, cells, LANES), f32)], [VMEM] * 3, [],
        tokens * slots, (table_first, table_own, table_second),
    )
    one = ((cells + FEATURES, tokens), f32)
    three = ((3, cells + FEATURES, tokens), f32)
    count_scratch = [vmem((tiles, slots + 8, LANES), i32)] * 2
    own = call(
        functools.partial(own_counts_kernel, cells), "own_counts", [one] * 3, [VMEM],
        count_scratch, pairs * 40, (packed,),
    )
    to_first, mid, to_second = call(
        functools.partial(counts_kernel, cells), "counts", [three] * 3, [VMEM] * 5 + [ANY],
        count_scratch, pairs * 80, (row_first, row_second, *own, ltp),
    )
    from_first, from_second = swapped(to_first, to_second, "col")

    logs = (tiles, LANES)
    parts, = call(
        row_parts_kernel, "row_parts", [((group, padded_to(3 * tiles, 8), LANES), f32)], [VMEM] * 5,
        [
            vmem((3,) + logs, f32),
            vmem((3, PARTS * cells, tokens), f32),
            vmem((3, cells, tokens), f32),
        ],
        pairs * 100,
        (to_first, mid, to_second, ltp, par),
    )
    told = lax.all_to_all(parts, ("row", "col"), 0, 0)

    x = (from_first, mid, from_second)
    sum_scratch = [
        vmem((3, cells, tokens), bf16),
        vmem((6, cells, LANES), f32),
        vmem((padded, cells), f32),
    ]
    e, m, held, parts, state_own = call(
        functools.partial(middle_kernel, gene_total), "middle",
        [
            ((3, 3, cells, tokens), f32),
            ((3, 3) + logs, f32),
            ((3, 3) + logs, f32),
            ((group, 6 * tiles, LANES), f32),
            state,
        ],
        [VMEM] * 7,
        [vmem((3, 3, padded, tokens), bf16)] + sum_scratch + [
            vmem((PARTS * cells, padded), bf16),
            vmem((6, cells, LANES), f32),
            vmem((3, PARTS * cells, tokens), f32),
            vmem((3, cells, tokens), f32),
            vmem(*table),
            vmem((3, 3) + logs, f32),
        ],
        pairs * 200,
        (*x, ltp, par, state_own, told),
    )
    told = lax.all_to_all(parts, ("row", "col"), 0, 0)
    final_profile, final_cells = call(
        functools.partial(last_kernel, gene_total), "last",
        [((gene_total, cells), f32), ((6, 1, cells), f32)],
        [VMEM] * 8, sum_scratch + [vmem((3, 3) + logs, f32)], pairs * 100,
        (*x, e, m, held, told, state_own),
    )
    return (final_profile.reshape(gene_total, 1, 1, cells), final_cells.reshape(6, 1, 1, cells))


def solution(mesh):
    tiles = P(("groups", "row"), "col")
    stacked = P(None, ("groups", "row"), "col", None)
    return jax.shard_map(
        body,
        mesh=mesh,
        in_specs=(
            stacked,
            P(("groups", "row"), "col", None),
            P(("groups", "row"), "col", None, None),
            P(("groups", "row"), "col", None),
            stacked,
            stacked,
            stacked,
            P(("groups", "row"), "col", None),
        ),
        out_specs=(stacked, stacked),
        check_vma=False,
    )
```

```python
import functools

import jax
import jax.numpy as jnp
from jax import lax
from jax.experimental import pallas as pl
from jax.experimental.pallas import tpu as pltpu
from jax.sharding import PartitionSpec as P


BLOCK = 256
LANES = 128
FEATURES = 8
PARTS = 2
NEVER = -1e30

pseudo_count = 0.05
prior_weight = 1.0

f32 = jnp.float32
bf16 = jnp.bfloat16
i32 = jnp.int32


def swapped(to_first, to_second, axis):
    count = lax.axis_size(axis)
    out = []
    for start, x in enumerate((to_first, to_second)):
        pairs = [p for i in range(start, count - 1, 2) for p in ((i, i + 1), (i + 1, i))]
        out.append(lax.ppermute(x, axis, pairs))
    return out


def params(mib=40):
    return pltpu.CompilerParams(vmem_limit_bytes=mib << 20)


def cost(flops, size):
    return pl.CostEstimate(flops=flops, bytes_accessed=size, transcendentals=0)


def call(kernel, outs, in_specs, scratch, flops, args):
    shapes = [jax.ShapeDtypeStruct(s, d) for s, d in outs]
    return pl.pallas_call(
        kernel,
        out_shape=shapes,
        in_specs=in_specs,
        out_specs=[pl.BlockSpec(memory_space=pltpu.VMEM)] * len(shapes),
        scratch_shapes=scratch,
        compiler_params=params(),
        cost_estimate=cost(flops, 1 << 20),
    )(*args)


VMEM = pl.BlockSpec(memory_space=pltpu.VMEM)
SMEM = pl.BlockSpec(memory_space=pltpu.SMEM)
ANY = pl.BlockSpec(memory_space=pltpu.HBM)


def lane_tile(k):
    return pl.ds(k * LANES, LANES)


def padded_to(size, unit):
    return -(-size // unit) * unit


def order(axis):
    first = 2 * (1 - lax.rem(lax.axis_index(axis), 2))
    return (first, 1, 2 - first)


def as_float(x):
    return x.astype(f32) if hasattr(x, "astype") else float(x)


def table_rows(profile, state, log_weight):
    genes, cells = profile.shape
    mu_row, mu_col, rr, rc, cc = state
    det = rr * cc - rc * rc
    rows = [jnp.log(profile)]
    if genes % 8:
        rows.append(jnp.zeros((-genes % 8, cells), f32))
    rows += [
        mu_row,
        mu_col,
        -0.5 * (cc / det),
        rc / det,
        -0.5 * (rr / det),
        log_weight - 0.5 * jnp.log(det),
        jnp.zeros((2, cells), f32),
    ]
    return jnp.concatenate(rows, axis=0)


def state_rows(state):
    return jnp.concatenate(list(state) + [jnp.zeros((3, state[0].shape[1]), f32)], axis=0)


def pack_kernel(
    count_hbm, cand_hbm, pos_hbm, gene_hbm, weight_hbm, centre_hbm, spread_hbm, corr_hbm,
    out_ref, table_ref, state_ref,
    count_ref, cand_ref, pos_ref, gene_ref, weight_ref, centre_ref, spread_ref, corr_ref, sems,
):
    pairs = (
        (count_hbm, count_ref), (cand_hbm, cand_ref), (pos_hbm, pos_ref), (gene_hbm, gene_ref), (weight_hbm, weight_ref),
        (centre_hbm, centre_ref), (spread_hbm, spread_ref), (corr_hbm, corr_ref),
    )
    copies = [pltpu.make_async_copy(a, b, sems.at[n]) for n, (a, b) in enumerate(pairs)]
    for copy in copies:
        copy.start()
    for copy in copies[:4]:
        copy.wait()
    tokens, slots = cand_ref.shape
    tiles = tokens // LANES
    out_ref[0:slots, :] = cand_ref[...].astype(f32).T
    lane = lax.broadcasted_iota(i32, (1, LANES), 1)
    for k in range(tiles):
        start = k * LANES
        live = (start % BLOCK + lane) < count_ref[:, start // BLOCK : start // BLOCK + 1]
        rows = [
            pos_ref[k : k + 1, :],
            pos_ref[tiles + k : tiles + k + 1, :],
            gene_ref[k : k + 1, :].astype(f32),
            live.astype(f32),
            jnp.zeros((FEATURES - 4, LANES), f32),
        ]
        out_ref[slots : slots + FEATURES, lane_tile(k)] = jnp.concatenate(rows, axis=0)
    for copy in copies[4:]:
        copy.wait()
    weights = weight_ref[...]
    spread_row, spread_col = spread_ref[0:1, :], spread_ref[1:2, :]
    state = (
        centre_ref[0:1, :],
        centre_ref[1:2, :],
        spread_row * spread_row,
        corr_ref[0:1, :] * spread_row * spread_col,
        spread_col * spread_col,
    )
    state_ref[...] = state_rows(state)
    profile = weights / jnp.sum(weights, axis=0, keepdims=True)
    table_ref[...] = table_rows(profile, state, jnp.zeros_like(spread_row))


def full_add(a, b, c):
    both = a ^ b
    return both ^ c, (a & b) | (both & c)


def count_source(source, z_ref, cells, outs, word_s, unit_s):
    rows, tokens = z_ref.shape
    slots = rows - FEATURES
    shift = cells.bit_length() - 1
    held = cells // 64
    planes = slots.bit_length()
    sub = lax.broadcasted_iota(i32, (8, LANES), 0)
    first = order("col")[0]
    for k in range(tokens // LANES):
        local = z_ref[0:slots, lane_tile(k)].astype(i32) - (2 - source) * 3 * cells
        tile = first + (local >> shift) * (1 - first)
        cell = local & (cells - 1)
        live = z_ref[slots + 3 : slots + 4, lane_tile(k)] > 0.0
        named = (tile >= 0) & (tile < 3) & live
        word_s[k, 0:slots, :] = ((cell >> 6) << 3) | (cell & 7)
        unit_s[k, 0:slots, :] = jnp.where(named, 1 << (((tile & 3) << 3) | ((cell >> 3) & 7)), 0)

    for k in range(tokens // LANES):

        def group(g, carry):
            bits = [[] for _ in range(held)]
            for j in range(16):
                which = word_s[k, pl.ds(g * 16 + j, 8, stride=0), :]
                unit = unit_s[k, pl.ds(g * 16 + j, 8, stride=0), :]
                for n in range(held):
                    bits[n].append(jnp.where(which == sub + 8 * n, unit, 0))
            out = []
            for n in range(held):
                plane = list(carry[n])
                level = bits[n]
                for p in range(4):
                    following = []
                    for a in range(0, len(level), 2):
                        plane[p], over = full_add(plane[p], level[a], level[a + 1])
                        following.append(over)
                    level = following
                over = level[0]
                for p in range(4, planes):
                    plane[p], over = plane[p] ^ over, plane[p] & over
                out.append(plane)
            return out

        zero = jnp.zeros((8, LANES), i32)
        total = lax.fori_loop(0, slots // 16, group, [[zero] * planes for _ in range(held)], unroll=True)
        for n in range(held):
            for r in range(8):
                value = zero
                for p in range(planes):
                    moved = total[n][p]
                    if r > p:
                        moved = moved >> (r - p)
                    elif r < p:
                        moved = moved << (p - r)
                    value = value | (moved & (0x00010101 << p))
                row = n * 64 + r * 8
                for tile, out in enumerate(outs):
                    part = value & 255 if tile == 0 else (value >> (8 * tile)) & 255
                    out[row : row + 8, lane_tile(k)] = part.astype(f32)
    for out in outs:
        out[cells : cells + FEATURES, :] = z_ref[slots : slots + FEATURES, :]


def own_counts_kernel(cells, own_ref, first_ref, mid_ref, second_ref, word_s, unit_s):
    count_source(1, own_ref, cells, (first_ref, mid_ref, second_ref), word_s, unit_s)


def counts_kernel(
    cells, first_ref, second_ref, own_first, own_mid, own_second,
    to_first, mid_ref, to_second, word_s, unit_s,
):
    outs = (to_first, mid_ref, to_second)
    for out, own in zip(outs, (own_first, own_mid, own_second)):
        out[1] = own[...]
    first, _, second = order("row")
    for q, source, z_ref in ((0, first, first_ref), (2, second, second_ref)):
        count_source(source, z_ref, cells, [out.at[q] for out in outs], word_s, unit_s)


def load_table(table_ref, ltp_s, par_s):
    cells = table_ref.shape[1]
    padded = ltp_s.shape[1]
    genes = table_ref.shape[0] - 8
    logs = [table_ref[0:genes, :]]
    if padded > genes:
        logs.append(jnp.zeros((padded - genes, cells), f32))
    rest = jnp.concatenate(logs, axis=0).T
    for part in range(PARTS):
        piece = rest.astype(bf16)
        ltp_s[part * cells : (part + 1) * cells, :] = piece
        if part + 1 < PARTS:
            rest = rest - piece.astype(f32)
    rows = [table_ref[genes : genes + 8, :], jnp.zeros((LANES - 8, cells), f32)]
    columns = jnp.concatenate(rows, axis=0).T
    for n in range(6):
        par_s[n] = jnp.broadcast_to(columns[:, n : n + 1], (cells, LANES))


def tables_kernel(first_ref, own_ref, second_ref, ltp_ref, par_ref):
    for side, table in enumerate((first_ref, own_ref, second_ref)):
        load_table(table, ltp_ref.at[side], par_ref.at[side])


def gene_hot(x_ref, source, cells, padded):
    tokens = x_ref.shape[2]
    gene = x_ref[source, cells + 2 : cells + 3, :].astype(i32).astype(jnp.int16)
    axis = lax.broadcasted_iota(jnp.int16, (padded, tokens), 0)
    return jnp.where(axis == gene, jnp.ones((), bf16), jnp.zeros((), bf16))


def features(x_ref, source, cells, row_step, col_step):
    y0 = x_ref[source, cells : cells + 1, :] + row_step
    y1 = x_ref[source, cells + 1 : cells + 2, :] + col_step
    return y0, y1


def score_rows(at, y0, y1, gl_s, par_s, cells):
    tiles = y0.shape[1] // LANES
    p = [jnp.concatenate([par_s[n, at : at + 8, :]] * tiles, axis=1) for n in range(6)]
    d0 = y0 - p[0]
    d1 = y1 - p[1]
    logs = gl_s[at : at + 8, :]
    for part in range(1, PARTS):
        logs = logs + gl_s[part * cells + at : part * cells + at + 8, :]
    return logs + p[5] + (d0 * (p[2] * d0 + p[3] * d1) + p[4] * d1 * d1)


def row_of(ref, index, first, tiles):
    return jnp.concatenate([ref[index + (pl.ds(first + k, 1), slice(None))] for k in range(tiles)], axis=1)


def to_tiles(row):
    return jnp.concatenate([row[:, k * LANES : (k + 1) * LANES] for k in range(row.shape[1] // LANES)], axis=0)


def log_sum(top, total):
    return jnp.where(total > 0.0, top + jnp.log(total), NEVER)


def joined(parts):
    top = functools.reduce(jnp.maximum, parts)
    return top + jnp.log(sum(jnp.exp(p - top) for p in parts))


def device_at(row_step, col_step):
    rows, cols = lax.axis_size("row"), lax.axis_size("col")
    row = lax.axis_index("row") + row_step
    col = lax.axis_index("col") + col_step
    inside = (row >= 0) & (row < rows) & (col >= 0) & (col < cols)
    return inside, jnp.clip(row, 0, rows - 1) * cols + jnp.clip(col, 0, cols - 1)


def send_first(part_s, out_ref):
    cols = lax.axis_size("col")
    row = lax.axis_index("row")
    tiles = part_s.shape[1]

    @pl.loop(0, out_ref.shape[0] // cols)
    def _(at):
        for q in range(3):
            source = at - row + q
            inside = (source >= 0) & (source < 3)
            part = jnp.where(inside, part_s[jnp.clip(source, 0, 2)], NEVER)
            for c in range(cols):
                out_ref[at * cols + c, q * tiles : (q + 1) * tiles, :] = part


def receive_first(in_ref, log_s):
    tiles = log_s.shape[2]
    for q in range(3):
        for s in range(3):
            parts = []
            for row_step in range(q - 2, q + 1):
                inside, at = device_at(row_step, s - 1)
                parts.append(jnp.where(inside, in_ref[at, q * tiles : (q + 1) * tiles, :], NEVER))
            log_s[q, s] = joined(parts)


def place(q, s, row_step, col_step):
    if row_step == 0:
        return q * 2 + s - max(0, -col_step)
    return (q - max(0, -row_step)) * 3 + s


def send_second(part_s, out_ref):
    tiles = part_s.shape[2]
    for row_step in range(-2, 3):
        for col_step in range(-2, 3):
            if row_step == 0 and col_step == 0:
                continue
            inside, at = device_at(row_step, col_step)

            @pl.when(inside)
            def _(row_step=row_step, col_step=col_step, at=at):
                for q in range(max(0, -row_step), min(3, 3 - row_step)):
                    for s in range(max(0, -col_step), min(3, 3 - col_step)):
                        slot = place(q, s, row_step, col_step) * tiles
                        out_ref[at, slot : slot + tiles, :] = part_s[q + row_step, s + col_step]


def receive_second(in_ref, own_ref, log_s):
    tiles = log_s.shape[2]
    for q in range(3):
        for s in range(3):
            parts = [own_ref[q, s]]
            for row_step in range(q - 2, q + 1):
                for col_step in range(s - 2, s + 1):
                    if row_step == 0 and col_step == 0:
                        continue
                    inside, at = device_at(row_step, col_step)
                    slot = place(q, s, -row_step, -col_step) * tiles
                    parts.append(jnp.where(inside, in_ref[at, slot : slot + tiles, :], NEVER))
            log_s[q, s] = joined(parts)


def row_parts_kernel(
    first_ref, mid_ref, second_ref, ltp_s, par_s, out_ref, part_s, gl_s, sc_s
):
    x_refs = (first_ref, mid_ref, second_ref)
    cells, tokens = sc_s.shape[1:]

    for q, source in enumerate(order("row")):
        hot = gene_hot(mid_ref, q, cells, ltp_s.shape[2])
        for side in range(3):
            gl_s[side] = jnp.dot(ltp_s[side], hot, preferred_element_type=f32)
        top = jnp.full((8, tokens), NEVER, f32)
        for side, at_side in enumerate(order("col")):
            y0, y1 = features(mid_ref, q, cells, as_float(source) - 1.0, 1.0 - as_float(at_side))
            for at in range(0, cells, 8):
                score = score_rows(at, y0, y1, gl_s.at[side], par_s.at[side], cells)
                score = jnp.where(x_refs[side][q, at : at + 8, :] > 0.0, score, NEVER)
                sc_s[side, at : at + 8, :] = score
                top = jnp.maximum(top, score)
        top = jnp.max(top, axis=0, keepdims=True)
        total = jnp.zeros((8, tokens), f32)
        for side in range(3):
            for at in range(0, cells, 8):
                count = x_refs[side][q, at : at + 8, :]
                total = total + count * jnp.exp(sc_s[side, at : at + 8, :] - top)
        total = jnp.sum(total, axis=0, keepdims=True)
        part_s[source] = to_tiles(log_sum(top, total))
    send_first(part_s, out_ref)


def add_moments(p, y0, y1, sums):
    def fold(x):
        parts = [x[:, k * LANES : (k + 1) * LANES] for k in range(x.shape[1] // LANES)]
        return functools.reduce(jnp.add, parts)

    weights = (None, y0, y1, y0 * y0, y0 * y1, y1 * y1)
    return [s + fold(p if w is None else p * w) for s, w in zip(sums, weights)]


def add_counts(hot, sh_s, cnt_s):
    cnt_s[...] += lax.dot_general(hot, sh_s[...], (((1,), (1,)), ((), ())), preferred_element_type=f32)


def new_cells(genes, mom_s, cnt_s, state_ref):
    weight, s0, s1, s00, s01, s11 = [jnp.sum(mom_s[n].T, axis=0, keepdims=True) for n in range(6)]
    mu_row, mu_col, rr, rc, cc = [state_ref[n : n + 1, :] for n in range(5)]
    counts = cnt_s[0:genes, :]
    profile = (counts + pseudo_count) / (
        jnp.sum(counts, axis=0, keepdims=True) + genes * pseudo_count
    )
    denominator = weight + prior_weight
    new_row = (s0 + prior_weight * mu_row) / denominator
    new_col = (s1 + prior_weight * mu_col) / denominator
    q_rr = s00 - 2.0 * new_row * s0 + weight * new_row * new_row
    q_rc = s01 - new_row * s1 - new_col * s0 + weight * new_row * new_col
    q_cc = s11 - 2.0 * new_col * s1 + weight * new_col * new_col
    state = (
        new_row,
        new_col,
        (q_rr + prior_weight * rr) / denominator,
        (q_rc + prior_weight * rc) / denominator,
        (q_cc + prior_weight * cc) / denominator,
    )
    return profile, state, jnp.log(weight + 1.0)


def middle_kernel(
    genes,
    first_ref, mid_ref, second_ref, ltp_ref, par_ref, state_ref, told_ref,
    e_ref, m_ref, part_ref, out_ref, state_out,
    hot_s, sh_s, mom_s, cnt_s, ltp_s, par_s, gl_s, sc_s, table_s, log_s,
):
    x_refs = (first_ref, mid_ref, second_ref)
    cells, tokens = sc_s.shape[1:]
    tiles = tokens // LANES
    padded = cnt_s.shape[0]
    mom_s[...] = jnp.zeros(mom_s.shape, f32)
    cnt_s[...] = jnp.zeros(cnt_s.shape, f32)
    receive_first(told_ref, log_s)

    for q, source in enumerate(order("row")):
        for side, x_ref in enumerate(x_refs):
            hot_s[q, side] = gene_hot(x_ref, q, cells, padded)
            gl_s[side] = jnp.dot(ltp_ref[1], hot_s[q, side], preferred_element_type=f32)
        for side, (at_side, x_ref) in enumerate(zip(order("col"), x_refs)):
            total = row_of(log_s, (source, at_side), 0, tiles)
            y0, y1 = features(x_ref, q, cells, as_float(source) - 1.0, as_float(at_side) - 1.0)
            for at in range(0, cells, 16):
                halves = []
                for a in (at, at + 8):
                    score = score_rows(a, y0, y1, gl_s.at[side], par_ref.at[1], cells)
                    count = x_ref[q, a : a + 8, :]
                    p = count * jnp.exp(jnp.minimum(score - total, 0.0))
                    sums = [mom_s[n, a : a + 8, :] for n in range(6)]
                    sums = add_moments(p, y0, y1, sums)
                    for n in range(6):
                        mom_s[n, a : a + 8, :] = sums[n]
                    halves.append(p)
                sh_s[side, at : at + 16, :] = jnp.concatenate(halves, axis=0).astype(bf16)
            add_counts(hot_s[q, side], sh_s.at[side], cnt_s)

    profile, state, log_weight = new_cells(genes, mom_s, cnt_s, state_ref)
    state_out[...] = state_rows(state)
    table_s[...] = table_rows(profile, state, log_weight)
    load_table(table_s, ltp_s, par_s)

    for q, source in enumerate(order("row")):
        for side in range(3):
            gl_s[side] = jnp.dot(ltp_s[...], hot_s[q, side], preferred_element_type=f32)
        for side, (at_side, x_ref) in enumerate(zip(order("col"), x_refs)):
            y0, y1 = features(x_ref, q, cells, as_float(source) - 1.0, as_float(at_side) - 1.0)
            top = jnp.full((8, tokens), NEVER, f32)
            for at in range(0, cells, 8):
                value = score_rows(at, y0, y1, gl_s.at[side], par_s, cells)
                value = jnp.where(x_ref[q, at : at + 8, :] > 0.0, value, NEVER)
                sc_s[side, at : at + 8, :] = value
                top = jnp.maximum(top, value)
            top = jnp.max(top, axis=0, keepdims=True)
            total = jnp.zeros((8, tokens), f32)
            for at in range(0, cells, 8):
                e = x_ref[q, at : at + 8, :] * jnp.exp(sc_s[side, at : at + 8, :] - top)
                e_ref[q, side, at : at + 8, :] = e
                total = total + e
            total = jnp.sum(total, axis=0, keepdims=True)
            m_ref[source, at_side] = to_tiles(top)
            part_ref[source, at_side] = to_tiles(log_sum(top, total))

    send_second(part_ref, out_ref)


def last_kernel(
    genes,
    first_ref, mid_ref, second_ref, e_ref, m_ref, part_ref, told_ref, state_ref,
    profile_ref, cells_ref,
    sh_s, mom_s, cnt_s, log_s,
):
    x_refs = (first_ref, mid_ref, second_ref)
    cells, tokens = sh_s.shape[1:]
    tiles = tokens // LANES
    mom_s[...] = jnp.zeros(mom_s.shape, f32)
    cnt_s[...] = jnp.zeros(cnt_s.shape, f32)
    receive_second(told_ref, part_ref, log_s)

    for q, source in enumerate(order("row")):
        for side, (at_side, x_ref) in enumerate(zip(order("col"), x_refs)):
            scale = jnp.exp(m_ref[source, at_side] - log_s[source, at_side])
            factor = jnp.concatenate([scale[k : k + 1, :] for k in range(tiles)], axis=1)
            y0, y1 = features(x_ref, q, cells, as_float(source) - 1.0, as_float(at_side) - 1.0)
            for at in range(0, cells, 16):
                halves = []
                for a in (at, at + 8):
                    p = e_ref[q, side, a : a + 8, :] * factor
                    sums = [mom_s[n, a : a + 8, :] for n in range(6)]
                    sums = add_moments(p, y0, y1, sums)
                    for n in range(6):
                        mom_s[n, a : a + 8, :] = sums[n]
                    halves.append(p)
                sh_s[side, at : at + 16, :] = jnp.concatenate(halves, axis=0).astype(bf16)
            add_counts(gene_hot(x_ref, q, cells, cnt_s.shape[0]), sh_s.at[side], cnt_s)

    profile, state, log_weight = new_cells(genes, mom_s, cnt_s, state_ref)
    profile_ref[...] = jnp.log(profile)
    mu_row, mu_col, rr, rc, cc = state
    final = (mu_row, mu_col, 0.5 * jnp.log(rr), 0.5 * jnp.log(cc), rc / jnp.sqrt(rr * cc), log_weight)
    for n, row in enumerate(final):
        cells_ref[n] = row


def body(
    positions, genes, candidates, block_counts, profile_weights, centroids, spreads, correlation
):
    gene_total = profile_weights.shape[0]
    cells = profile_weights.shape[3]
    tokens, slots = candidates.shape[2:]
    tiles = tokens // LANES
    group = lax.axis_size("row") * lax.axis_size("col")
    padded = padded_to(gene_total, LANES)
    pairs = 9 * tokens * cells
    table = ((padded_to(gene_total, 8) + 8, cells), f32)
    state = ((8, cells), f32)
    vmem = pltpu.VMEM

    packed, table_own, state_own = call(
        pack_kernel, [((slots + FEATURES, tokens), f32), table, state],
        [ANY] * 8,
        [
            vmem((1, block_counts.shape[2]), i32),
            vmem((tokens, slots), i32),
            vmem((2 * tiles, LANES), f32),
            vmem((tiles, LANES), i32),
            vmem((gene_total, cells), f32),
            vmem((2, cells), f32),
            vmem((2, cells), f32),
            vmem((1, cells), f32),
            pltpu.SemaphoreType.DMA((8,)),
        ],
        tokens * slots,
        [
            pltpu.with_memory_space_constraint(a, pltpu.HBM)
            for a in (
                block_counts.reshape(1, -1),
                candidates.reshape(tokens, slots),
                positions.reshape(2 * tiles, LANES),
                genes.reshape(tiles, LANES),
                profile_weights.reshape(gene_total, cells),
                centroids.reshape(2, cells),
                spreads.reshape(2, cells),
                correlation.reshape(1, cells),
            )
        ],
    )
    row_first, row_second = swapped(packed, packed, "row")
    table_first, table_second = swapped(table_own, table_own, "col")
    ltp, par = call(
        tables_kernel,
        [((3, PARTS * cells, padded), bf16), ((3, 6, cells, LANES), f32)], [VMEM] * 3, [],
        tokens * slots, (table_first, table_own, table_second),
    )
    one = ((cells + FEATURES, tokens), f32)
    three = ((3, cells + FEATURES, tokens), f32)
    count_scratch = [vmem((tiles, slots + 8, LANES), i32)] * 2
    own = call(
        functools.partial(own_counts_kernel, cells), [one] * 3, [VMEM],
        count_scratch, pairs * 40, (packed,),
    )
    to_first, mid, to_second = call(
        functools.partial(counts_kernel, cells), [three] * 3, [VMEM] * 5,
        count_scratch, pairs * 80, (row_first, row_second, *own),
    )
    from_first, from_second = swapped(to_first, to_second, "col")

    logs = (tiles, LANES)
    parts, = call(
        row_parts_kernel, [((group, padded_to(3 * tiles, 8), LANES), f32)], [VMEM] * 5,
        [
            vmem((3,) + logs, f32),
            vmem((3, PARTS * cells, tokens), f32),
            vmem((3, cells, tokens), f32),
        ],
        pairs * 100,
        (to_first, mid, to_second, ltp, par),
    )
    told = lax.all_to_all(parts, ("row", "col"), 0, 0)

    x = (from_first, mid, from_second)
    sum_scratch = [
        vmem((3, cells, tokens), bf16),
        vmem((6, cells, LANES), f32),
        vmem((padded, cells), f32),
    ]
    e, m, held, parts, state_own = call(
        functools.partial(middle_kernel, gene_total),
        [
            ((3, 3, cells, tokens), f32),
            ((3, 3) + logs, f32),
            ((3, 3) + logs, f32),
            ((group, 6 * tiles, LANES), f32),
            state,
        ],
        [VMEM] * 7,
        [vmem((3, 3, padded, tokens), bf16)] + sum_scratch + [
            vmem((PARTS * cells, padded), bf16),
            vmem((6, cells, LANES), f32),
            vmem((3, PARTS * cells, tokens), f32),
            vmem((3, cells, tokens), f32),
            vmem(*table),
            vmem((3, 3) + logs, f32),
        ],
        pairs * 200,
        (*x, ltp, par, state_own, told),
    )
    told = lax.all_to_all(parts, ("row", "col"), 0, 0)
    final_profile, final_cells = call(
        functools.partial(last_kernel, gene_total),
        [((gene_total, cells), f32), ((6, 1, cells), f32)],
        [VMEM] * 8, sum_scratch + [vmem((3, 3) + logs, f32)], pairs * 100,
        (*x, e, m, held, told, state_own),
    )
    return (final_profile.reshape(gene_total, 1, 1, cells), final_cells.reshape(6, 1, 1, cells))


def solution(mesh):
    stacked = P(None, ("groups", "row"), "col", None)

    return jax.shard_map(
        body,
        mesh=mesh,
        in_specs=(
            stacked,
            P(("groups", "row"), "col", None),
            P(("groups", "row"), "col", None, None),
            P(("groups", "row"), "col", None),
            stacked,
            stacked,
            stacked,
            P(("groups", "row"), "col", None),
        ),
        out_specs=(stacked, stacked),
        check_vma=False,
    )
```
